32 devices in a mesh: gx: 8 (over z, x), gy: 4 (over y, core).
Axes of the slice: x: 2, y: 2, z: 4, core: 2. Of those that a mesh axis runs over, the one named last changes fastest.
Arguments:
- populations: float32 [19, 64, 256, 256], P(None, 'gx', 'gy'), may hold values from 0 to 0.6
- rotation_init: float32 [3], replicated, may hold values from -0.75 to 0.75
- slot_cell: int32 [3, 8, 4, 2048], P(None, 'gx', 'gy'), may hold values from 0 to 255, as said below
- slot_count: int32 [8, 4], P('gx', 'gy'), may hold values from 128 to 2048, as said below
- marker_arm: float32 [3, 8, 4, 2048], P(None, 'gx', 'gy'), may hold values from -1.7 to 1.7
- marker_area: float32 [8, 4, 2048], P('gx', 'gy'), may hold values from 0.3 to 3
- marker_fraction: float32 [8, 4, 2048], P('gx', 'gy'), may hold values from 0 to 1
Outputs:
- populations_next: float32 [19, 64, 256, 256], P(None, 'gx', 'gy')
- rotation: float32 [3, 3], replicated
The draws below stay inside these ranges and needn't reach their ends.
Inputs may be any that keep to these rules, and one draw needn't show every extreme that they name: `slot_cell`: slot s of slab (a, b) names a cell whose first coordinate lies in [a * 8, (a + 1) * 8) and whose second lies in [b * 64, (b + 1) * 64); the third is any; slots at or past slot_count hold cells too but carry no marker. `slot_count`: some slab has all 2048 slots live in every draw.
All inputs are finite; a program needn't handle non-finite values.
Results may differ from the reference program's by a relative error of at most 0.0001.
Values sent between devices are 32-bit elements; how exact they have to be, the bound alone decides.
A program may use at most 128 MiB of HBM per device.

```python
import math
import jax
import jax.numpy as jnp
from jax import lax

Q = 19
CX = 8
CY = 64
NZ = 256
SLOTS = 2048
ITERS = 3
SLABS_X = 8
SLABS_Y = 4
NX = 64
NY = 256


VELOCITY_TABLE = ((0, 0, 0), (1, 0, 0), (-1, 0, 0), (0, 1, 0), (0, -1, 0), (0, 0, 1), (0, 0, -1), (1, 1, 0), (-1, -1, 0), (1, -1, 0), (-1, 1, 0), (1, 0, 1), (-1, 0, -1), (1, 0, -1), (-1, 0, 1), (0, 1, 1), (0, -1, -1), (0, 1, -1), (0, -1, 1))


WEIGHT_TABLE = (1.0 / 3.0,) + (1.0 / 18.0,) * 6 + (1.0 / 36.0,) * 12


def marker_cells(key):
    extent = (SLABS_X, SLABS_Y, SLOTS)
    slab_extent = (SLABS_X, SLABS_Y, 1)
    subkeys = jax.random.split(jax.random.fold_in(key, 11), 5)
    span_y = min(CY, 16)
    span_z = min(NZ, max(1, SLOTS // (CX * span_y)))
    slab_x = lax.broadcasted_iota(jnp.int32, extent, 0)
    slab_y = lax.broadcasted_iota(jnp.int32, extent, 1)
    start_y = jax.random.randint(subkeys[0], slab_extent, 0, CY - span_y + 1)
    start_z = jax.random.randint(subkeys[1], slab_extent, 0, NZ - span_z + 1)
    coord_x = slab_x * CX + jax.random.randint(subkeys[2], extent, 0, CX)
    coord_y = slab_y * CY + start_y + jax.random.randint(subkeys[3], extent, 0, span_y)
    coord_z = start_z + jax.random.randint(subkeys[4], extent, 0, span_z)
    return jnp.stack([coord_x, coord_y, coord_z]).astype(jnp.int32)


def unit_vector(key):
    halves = jax.random.split(key, 2)
    height = jax.random.uniform(halves[0], (), jnp.float32, -1.0, 1.0)
    azimuth = jax.random.uniform(halves[1], (), jnp.float32, -math.pi, math.pi)
    radius = jnp.sqrt(jnp.maximum(1.0 - height * height, 0.0))
    return jnp.stack([radius * jnp.cos(azimuth), radius * jnp.sin(azimuth), height])


def draw_populations(key, part):
    extent = (NX, NY, NZ)
    lengths = (NX, NY, NZ)
    subkeys = jax.random.split(jax.random.fold_in(key, 53), 4)
    places = [(lax.broadcasted_iota(jnp.float32, extent, number) + 0.5 - 0.5 * lengths[number]) / (0.5 * lengths[number]) for number in range(3)]
    spin_axis = unit_vector(subkeys[0])
    swirling = [spin_axis[1] * places[2] - spin_axis[2] * places[1], spin_axis[2] * places[0] - spin_axis[0] * places[2], spin_axis[0] * places[1] - spin_axis[1] * places[0]]
    offset_flow = jnp.zeros((3,), jnp.float32)
    mean_flow = [0.15 * swirling[number] + offset_flow[number] for number in range(3)]
    density = jax.random.uniform(subkeys[2], extent, jnp.float32, 0.8, 1.2)
    speed_sq = mean_flow[0] * mean_flow[0] + mean_flow[1] * mean_flow[1] + mean_flow[2] * mean_flow[2]
    members = []
    for member in range(19):
        step_x, step_y, step_z = VELOCITY_TABLE[member]
        projected = step_x * mean_flow[0] + step_y * mean_flow[1] + step_z * mean_flow[2]
        noise_key = jax.random.fold_in(subkeys[3], member)
        jitter = jax.random.uniform(noise_key, extent, jnp.float32, -0.3, 0.3)
        members.append(WEIGHT_TABLE[member] * density * (1.0 + 3.0 * projected + 4.5 * projected * projected - 1.5 * speed_sq) * (1.0 + jitter))
    return jnp.stack(members).astype(jnp.float32)


def draw_slot_cell(key, part):
    return marker_cells(key)


def draw_marker_arm(key, part):
    positions = marker_cells(key).astype(jnp.float32)
    extents = jnp.asarray([NX, NY, NZ], jnp.float32)[:, None, None, None]
    centred = (positions + 0.5 - 0.5 * extents) / (0.5 * extents)
    subkey = jax.random.fold_in(key, 41)
    jitter = 0.1 * jnp.clip(jax.random.normal(subkey, positions.shape, jnp.float32), -3.0, 3.0)
    result = centred + jitter
    return result.astype(jnp.float32)


def draw_slot_count(key, part):
    extent = (SLABS_X, SLABS_Y)
    subkeys = jax.random.split(jax.random.fold_in(key, 23), 4)
    sparse_count = jax.random.randint(subkeys[0], extent, SLOTS // 16, SLOTS // 3 + 1)
    dense_count = SLOTS - jax.random.randint(subkeys[1], extent, 0, SLOTS // 4 + 1)
    surface = jax.random.randint(subkeys[2], extent, 0, 4) == 0
    counts = jnp.where(surface, dense_count, sparse_count)
    chosen = jax.random.randint(subkeys[3], (), 0, SLABS_X * SLABS_Y)
    position = lax.broadcasted_iota(jnp.int32, extent, 0) * SLABS_Y + lax.broadcasted_iota(jnp.int32, extent, 1)
    return jnp.where(position == chosen, SLOTS, counts).astype(jnp.int32)


def draw_marker_area(key, part):
    extent = (SLABS_X, SLABS_Y, SLOTS)
    position = (lax.broadcasted_iota(jnp.int32, extent, 0) * SLABS_Y + lax.broadcasted_iota(jnp.int32, extent, 1)).astype(jnp.float32)
    growth = 1.0 + 2.0 * position / max(1, SLABS_X * SLABS_Y - 1)
    subkey = jax.random.fold_in(key, 37)
    sample = jnp.exp(jax.random.uniform(subkey, extent, jnp.float32, math.log(0.3), 0.0))
    return (sample * growth).astype(jnp.float32)


def levels(own_key, shape, pieces, least, largest):
    def one(dim, parts):
        steps = jax.random.uniform(jax.random.fold_in(jax.random.fold_in(own_key, 6), dim), (parts,), jnp.float32, least / len(pieces), largest / len(pieces))
        return jnp.repeat(jnp.exp(steps), shape[dim] // parts).reshape((-1,) + (1,) * (len(shape) - dim - 1))

    gain = one(*pieces[0])
    for cut in pieces[1:]:
        gain = gain * one(*cut)
    return gain


def bell_draw(own_key, dims, deviation, limit, dtype=jnp.bfloat16):
    values = deviation * jax.random.normal(own_key, dims, jnp.float32)
    return jnp.clip(values, min=-limit, max=limit).astype(dtype)


def setup_inputs(seed: int = 0) -> dict:
    streams_of = jax.random.split(jax.random.key(seed), 8)
    populations = draw_populations(jax.random.fold_in(streams_of[7], 71), 0)
    rotation_init = bell_draw(streams_of[1], (3,), 0.25, 0.75, jnp.float32)
    slot_cell = draw_slot_cell(jax.random.fold_in(streams_of[7], 71), 0)
    slot_count = draw_slot_count(jax.random.fold_in(streams_of[7], 71), 0)
    marker_arm = draw_marker_arm(jax.random.fold_in(streams_of[7], 71), 0)
    marker_area = draw_marker_area(jax.random.fold_in(streams_of[7], 71), 0)
    marker_fraction = jnp.clip(1.0 * jax.random.uniform(streams_of[6], (SLABS_X, SLABS_Y, SLOTS), jnp.float32) ** levels(streams_of[6], (SLABS_X, SLABS_Y, SLOTS), ((0, 8), (1, 4)), -0.2, 0.2), 0.0, 1.0)
    return {"populations": populations, "rotation_init": rotation_init, "slot_cell": slot_cell, "slot_count": slot_count, "marker_arm": marker_arm, "marker_area": marker_area, "marker_fraction": marker_fraction}


VELOCITY_TABLE = ((0, 0, 0), (1, 0, 0), (-1, 0, 0), (0, 1, 0), (0, -1, 0), (0, 0, 1), (0, 0, -1),
                  (1, 1, 0), (-1, -1, 0), (1, -1, 0), (-1, 1, 0), (1, 0, 1), (-1, 0, -1),
                  (1, 0, -1), (-1, 0, 1), (0, 1, 1), (0, -1, -1), (0, 1, -1), (0, -1, 1))
WEIGHT_TABLE = (1.0 / 3.0,) + (1.0 / 18.0,) * 6 + (1.0 / 36.0,) * 12
RELAX_TIME = 0.8
SPREAD_GAIN = 0.25
SPIN_GAIN = 0.5


def cross(first, second):
    return jnp.stack([first[1] * second[2] - first[2] * second[1],
                      first[2] * second[0] - first[0] * second[2],
                      first[0] * second[1] - first[1] * second[0]])


def reference(populations, rotation_init, slot_cell, slot_count, marker_arm, marker_area, marker_fraction):
    density = jnp.sum(populations, axis=0)
    momentum = []
    for axis_number in range(3):
        total = jnp.zeros_like(density)
        for member in range(Q):
            direction = VELOCITY_TABLE[member][axis_number]
            if direction != 0:
                total = total + direction * populations[member]
        momentum.append(total)
    velocity = jnp.stack(momentum) / density
    coord_x = slot_cell[0].reshape(-1).astype(jnp.int32)
    coord_y = slot_cell[1].reshape(-1).astype(jnp.int32)
    coord_z = slot_cell[2].reshape(-1).astype(jnp.int32)
    cell_low = (coord_x * NY + coord_y) * NZ + coord_z
    cell_high = (coord_x * NY + coord_y) * NZ + (coord_z + 1) % NZ
    active = lax.broadcasted_iota(jnp.int32, (SLABS_X, SLABS_Y, SLOTS), 2) < slot_count[:, :, None]
    weight = jnp.where(active, marker_area, jnp.zeros_like(marker_area)).reshape(-1)
    fraction = marker_fraction.reshape(-1)
    lever = marker_arm.reshape(3, -1)
    inertia = jnp.sum(weight * jnp.sum(lever * lever, axis=0))
    velocity_field = velocity.reshape(3, -1)
    spin = rotation_init
    history = []
    for step_index in range(ITERS):
        sampled = (1.0 - fraction) * velocity_field[:, cell_low] + fraction * velocity_field[:, cell_high]
        target = cross(spin[:, None], lever)
        impulse = weight * (target - sampled)
        velocity_field = velocity_field.at[:, cell_low].add(SPREAD_GAIN * (1.0 - fraction) * impulse)
        velocity_field = velocity_field.at[:, cell_high].add(SPREAD_GAIN * fraction * impulse)
        torque = -jnp.sum(cross(lever, impulse), axis=1)
        spin = spin + SPIN_GAIN * torque / inertia
        history.append(spin)
    velocity = velocity_field.reshape(3, NX, NY, NZ)
    speed_sq = jnp.sum(velocity * velocity, axis=0)
    outputs = []
    for member in range(Q):
        shift_x, shift_y, shift_z = VELOCITY_TABLE[member]
        projected = shift_x * velocity[0] + shift_y * velocity[1] + shift_z * velocity[2]
        equilibrium = WEIGHT_TABLE[member] * density * (1.0 + 3.0 * projected + 4.5 * projected * projected - 1.5 * speed_sq)
        relaxed = populations[member] - (populations[member] - equilibrium) / RELAX_TIME
        outputs.append(jnp.roll(relaxed, (shift_x, shift_y, shift_z), axis=(0, 1, 2)))
    return jnp.stack(outputs), jnp.stack(history)
```

```python
import functools

import jax
import jax.numpy as jnp
from jax import lax
from jax.experimental import pallas as pl
from jax.experimental.pallas import tpu as pltpu
from jax.sharding import PartitionSpec as P

Q = 19
ITERS = 3
VELOCITY_TABLE = (
    (0, 0, 0),
    (1, 0, 0),
    (-1, 0, 0),
    (0, 1, 0),
    (0, -1, 0),
    (0, 0, 1),
    (0, 0, -1),
    (1, 1, 0),
    (-1, -1, 0),
    (1, -1, 0),
    (-1, 1, 0),
    (1, 0, 1),
    (-1, 0, -1),
    (1, 0, -1),
    (-1, 0, 1),
    (0, 1, 1),
    (0, -1, -1),
    (0, 1, -1),
    (0, -1, 1),
)
WEIGHT_TABLE = (1.0 / 3.0,) + (1.0 / 18.0,) * 6 + (1.0 / 36.0,) * 12
RELAX_TIME = 0.8
SPREAD_GAIN = 0.25
SPIN_GAIN = 0.5
PLUS_X = [m for m in range(Q) if VELOCITY_TABLE[m][0] == 1]
MINUS_X = [m for m in range(Q) if VELOCITY_TABLE[m][0] == -1]
PLUS_Y = [m for m in range(Q) if VELOCITY_TABLE[m][1] == 1]
MINUS_Y = [m for m in range(Q) if VELOCITY_TABLE[m][1] == -1]
DIAGONAL = [m for m in range(Q) if VELOCITY_TABLE[m][0] != 0 and VELOCITY_TABLE[m][1] != 0]
MESH = pl.DeviceIdType.MESH
F32 = jnp.float32
BF16 = jnp.bfloat16
VMEM = pltpu.VMEM
VMEM_LIMIT = 60 * 1024 * 1024


def vmem():
    return pl.BlockSpec(memory_space=pltpu.VMEM)


def relax(member, value, density, velocity, common):
    direction = VELOCITY_TABLE[member]
    projected = None
    for number in range(3):
        if direction[number] != 0:
            term = velocity[number] if direction[number] > 0 else -velocity[number]
            projected = term if projected is None else projected + term
    scaled = density * (WEIGHT_TABLE[member] / RELAX_TIME)
    if projected is None:
        bracket = common
    else:
        bracket = common + projected * (3.0 + 4.5 * projected)
    return value * (1.0 - 1.0 / RELAX_TIME) + scaled * bracket


def common_of(velocity):
    squared = velocity[0] * velocity[0] + velocity[1] * velocity[1] + velocity[2] * velocity[2]
    return 1.0 - 1.5 * squared


def moments_kernel(pops_ref, density_ref, velocity_ref):
    depth = pops_ref.shape[3]
    values = [pops_ref[m, 0] for m in range(Q)]
    density = values[0]
    for m in range(1, Q):
        density = density + values[m]
    density_ref[...] = density
    for number in range(3):
        total = None
        for m in range(Q):
            direction = VELOCITY_TABLE[m][number]
            if direction != 0:
                if total is None:
                    total = values[m]
                else:
                    total = total + values[m] if direction > 0 else total - values[m]
        velocity_ref[:, number * depth : (number + 1) * depth] = total / density


def pieces_of(value, count):
    found = []
    for number in range(count):
        piece = value.astype(BF16)
        found.append(piece)
        if number < count - 1:
            value = value - piece.astype(F32)
    return found


def depth_table(depth, low, fraction):
    high = jnp.where(low == depth - 1.0, 0.0, low + 1.0)
    ids = lax.broadcasted_iota(jnp.int32, (depth, low.shape[1]), 0).astype(F32)
    return jnp.where(ids == low, 1.0 - fraction, 0.0) + jnp.where(ids == high, fraction, 0.0)


def plane_table(planes, row):
    ids = lax.broadcasted_iota(jnp.int32, (planes, row.shape[1]), 0).astype(F32)
    return jnp.where(ids == row, 1.0, 0.0).astype(BF16)


def gather_kernel(
    velocity_ref,
    pack_ref,
    sums_ref,
    linear_ref,
    turned_hi,
    turned_lo,
    state_ref,
    result_ref,
    cell_col,
    high_col,
    same_ref,
    after_ref,
    before_ref,
    left_ref,
):
    planes, triple = velocity_ref.shape
    depth = triple // 3
    slots = pack_ref.shape[1]
    turned = jnp.transpose(velocity_ref[...])
    hi, lo = pieces_of(turned, 2)
    turned_hi[...] = hi
    turned_lo[...] = lo
    chunk = 256
    steps = slots // chunk

    def gather(step, carry):
        at = pl.ds(pl.multiple_of(step * chunk, chunk), chunk)
        table = plane_table(planes, pack_ref[0:1, at])
        rows = jnp.dot(turned_hi[...], table, preferred_element_type=F32)
        rows = rows + jnp.dot(turned_lo[...], table, preferred_element_type=F32)
        tap = depth_table(depth, pack_ref[1:2, at], pack_ref[3:4, at])
        for number in range(3):
            part = rows[number * depth : (number + 1) * depth]
            state_ref[number : number + 1, at] = jnp.sum(part * tap, axis=0, keepdims=True)
        return carry

    lax.fori_loop(0, steps, gather, 0)
    state_ref[3:6, :] = pack_ref[4:7, :]
    state_ref[6:8, :] = jnp.zeros((2, slots), F32)

    low = pack_ref[1:2, :]
    high = jnp.where(low == depth - 1.0, 0.0, low + 1.0)
    base = pack_ref[0:1, :] * float(depth)
    cell_row = base + low
    high_row = base + high
    both = jnp.concatenate([cell_row, high_row, jnp.zeros((6, slots), F32)], axis=0)
    columns = jnp.transpose(both)
    cell_col[...] = jnp.broadcast_to(columns[:, 0:1], (slots, 128))
    high_col[...] = jnp.broadcast_to(columns[:, 1:2], (slots, 128))
    result_ref[6:8, :] = both[0:2]

    def prepare():
        weighted = state_ref[...] * pack_ref[2:3, :]
        share = pack_ref[3:4, :]
        stacked = jnp.concatenate([weighted * (1.0 - share), weighted * share], axis=0)
        left_ref[...] = jnp.concatenate(pieces_of(stacked, 3), axis=0)

    def apply(build):
        def one(step, carry):
            at = pl.ds(pl.multiple_of(step * chunk, chunk), chunk)
            if build:
                for half in range(chunk // 128):
                    part = pl.ds(pl.multiple_of(step * chunk + half * 128, 128), 128)
                    lanes = slice(half * 128, (half + 1) * 128)
                    cell = result_ref[6:7, part]
                    cell_high = result_ref[7:8, part]
                    same_ref[step, :, lanes] = jnp.where(cell_col[...] == cell, 1.0, 0.0).astype(BF16)
                    after_ref[step, :, lanes] = jnp.where(high_col[...] == cell, 1.0, 0.0).astype(BF16)
                    before_ref[step, :, lanes] = jnp.where(cell_col[...] == cell_high, 1.0, 0.0).astype(BF16)
            left = left_ref[...]

            def product(table):
                out = jnp.dot(left, table, preferred_element_type=F32)
                return out[0:16] + out[16:32] + out[32:48]

            same = product(same_ref[step])
            after = product(after_ref[step])
            before = product(before_ref[step])
            share = pack_ref[3:4, at]
            total = (1.0 - share) * (same[0:8] + after[8:16]) + share * (same[8:16] + before[0:8])
            result_ref[0:6, at] = SPREAD_GAIN * total[0:6]
            return carry

        lax.fori_loop(0, steps, one, 0)

    prepare()
    apply(True)
    arm = pack_ref[4:7, :]
    weight = pack_ref[2:3, :]
    first = state_ref[0:3, :]
    second = first - result_ref[0:3, :]
    carried = result_ref[3:6, :]
    state_ref[0:3, :] = second
    state_ref[3:6, :] = carried
    prepare()
    apply(False)
    third = second - result_ref[0:3, :]
    later = carried - result_ref[3:6, :]
    heavy = arm * weight
    rows = []
    for vector in (arm, carried, later):
        for a in range(3):
            rows.append(heavy[a : a + 1] * vector)
    for vector in (first, second, third):
        rows.append(heavy[1:2] * vector[2:3] - heavy[2:3] * vector[1:2])
        rows.append(heavy[2:3] * vector[0:1] - heavy[0:1] * vector[2:3])
        rows.append(heavy[0:1] * vector[1:2] - heavy[1:2] * vector[0:1])
    rows.append(jnp.zeros((4, slots), F32))
    table = jnp.concatenate(rows, axis=0)
    sums_ref[...] = jnp.broadcast_to(jnp.sum(table, axis=1, keepdims=True), sums_ref.shape)
    linear_ref[0:3, :] = heavy
    linear_ref[3:6, :] = weight * (first + second + third)
    linear_ref[6:9, :] = weight * (carried + later)
    linear_ref[9:12, :] = weight * carried
    linear_ref[12:16, :] = jnp.zeros((4, slots), F32)


def total_kernel(x_count, y_count, part_ref, out_ref, near, mine, far, near_send, near_recv, far_send, far_recv):
    x = lax.axis_index("gx")
    y = lax.axis_index("gy")
    barrier = pltpu.get_barrier_semaphore()
    for step in range(1, y_count):
        pl.semaphore_signal(barrier, inc=1, device_id=(x, lax.rem(y + step, y_count)), device_id_type=MESH)
    for step in range(1, x_count):
        pl.semaphore_signal(barrier, inc=1, device_id=(lax.rem(x + step, x_count), y), device_id_type=MESH)
    pl.semaphore_wait(barrier, x_count + y_count - 2)

    def near_copy(step):
        return pltpu.make_async_remote_copy(
            src_ref=part_ref,
            dst_ref=near.at[step - 1],
            send_sem=near_send.at[step - 1],
            recv_sem=near_recv.at[step - 1],
            device_id=(x, lax.rem(y + step, y_count)),
            device_id_type=MESH,
        )

    def far_copy(step):
        return pltpu.make_async_remote_copy(
            src_ref=mine,
            dst_ref=far.at[step - 1],
            send_sem=far_send.at[step - 1],
            recv_sem=far_recv.at[step - 1],
            device_id=(lax.rem(x + step, x_count), y),
            device_id_type=MESH,
        )

    def ordered(own, slots, count, position):
        total = None
        for source in range(count):
            value = own
            for step in range(1, count):
                hit = lax.rem(position + count - step, count) == source
                value = jnp.where(hit, slots[step - 1], value)
            total = value if total is None else total + value
        return total

    for step in range(1, y_count):
        near_copy(step).start()
    for step in range(1, y_count):
        near_copy(step).wait()
    mine[...] = ordered(part_ref[...], near, y_count, y)
    for step in range(1, x_count):
        far_copy(step).start()
    for step in range(1, x_count):
        far_copy(step).wait()
    out_ref[...] = ordered(mine[...], far, x_count, x)


def cross(first, second):
    return [
        first[1] * second[2] - first[2] * second[1],
        first[2] * second[0] - first[0] * second[2],
        first[0] * second[1] - first[1] * second[0],
    ]


def spread_kernel(
    rows_y,
    spin_ref,
    sums_ref,
    linear_ref,
    pack_ref,
    velocity_ref,
    density_ref,
    pops_ref,
    moved_ref,
    spins_ref,
    x_up_ref,
    x_down_ref,
    y_up_ref,
    y_down_ref,
    corner_a,
    corner_b,
    corner_c,
    corner_d,
    table_ref,
    hi_ref,
    lo_ref,
    x_in,
    y_in,
    x_sem,
    y_sem,
):
    planes, depth = density_ref.shape
    rows_x = planes // rows_y
    copies = []
    for number, m in enumerate(PLUS_X + MINUS_X):
        layer = rows_x - 1 if m in PLUS_X else 0
        copies.append(pltpu.make_async_copy(pops_ref.at[m, layer], x_in.at[number], x_sem.at[number]))
    for number, m in enumerate(PLUS_Y + MINUS_Y):
        row = rows_y - 1 if m in PLUS_Y else 0
        copies.append(pltpu.make_async_copy(pops_ref.at[m, :, row], y_in.at[number], y_sem.at[number]))
    for copy in copies:
        copy.start()

    def number_at(index):
        return sums_ref[index : index + 1, 0:1]

    def turning(offset, spin):
        entry = [[number_at(offset + a * 3 + b) for b in range(3)] for a in range(3)]
        trace = entry[0][0] + entry[1][1] + entry[2][2]
        return [
            spin[b] * trace - (entry[0][b] * spin[0] + entry[1][b] * spin[1] + entry[2][b] * spin[2])
            for b in range(3)
        ]

    inertia = number_at(0) + number_at(4) + number_at(8)
    spin = [spin_ref[0:1, number : number + 1] for number in range(3)]
    spins = [spin]
    spins_ref[...] = jnp.zeros(spins_ref.shape, F32)
    for step in range(ITERS):
        own = turning(0, spins[step])
        torque = [number_at(27 + step * 3 + b) - own[b] for b in range(3)]
        if step >= 1:
            back = turning(9, spins[step - 1])
            torque = [torque[b] + back[b] for b in range(3)]
        if step >= 2:
            back = turning(18, spins[step - 2])
            torque = [torque[b] + back[b] for b in range(3)]
        spins.append([spins[step][b] + SPIN_GAIN * torque[b] / inertia for b in range(3)])
        for b in range(3):
            spins_ref[step : step + 1, b : b + 1] = spins[step + 1][b]
    whole = [spins[0][b] + spins[1][b] + spins[2][b] for b in range(3)]

    def linear(start):
        return [linear_ref[start + b : start + b + 1, :] for b in range(3)]

    lead = cross(whole, linear(0))
    fall = linear(3)
    zeroth = cross(spins[0], linear(6))
    once = cross(spins[1], linear(9))
    impulse = [SPREAD_GAIN * (lead[b] - fall[b] - zeroth[b] - once[b]) for b in range(3)]
    table_ref[...] = plane_table(planes, pack_ref[0:1, :])
    tap = depth_table(depth, pack_ref[1:2, :], pack_ref[3:4, :])
    for number in range(3):
        lanes = slice(number * depth, (number + 1) * depth)
        hi, lo = pieces_of(tap * impulse[number], 2)
        hi_ref[...] = hi
        lo_ref[...] = lo
        dims = (((1,), (1,)), ((), ()))
        added = lax.dot_general(table_ref[...], hi_ref[...], dims, preferred_element_type=F32)
        added = added + lax.dot_general(table_ref[...], lo_ref[...], dims, preferred_element_type=F32)
        moved_ref[:, lanes] = velocity_ref[:, lanes] + added

    for copy in copies:
        copy.wait()

    def face(at, members, incoming, first):
        velocity = [moved_ref[at, number * depth : (number + 1) * depth] for number in range(3)]
        common = common_of(velocity)
        density = density_ref[at, :]
        return [
            relax(m, incoming[first + index], density, velocity, common)
            for index, m in enumerate(members)
        ]

    corners = {7: corner_a, 8: corner_b, 9: corner_c, 10: corner_d}
    for members, out, layer, first in (
        (PLUS_X, x_up_ref, rows_x - 1, 0),
        (MINUS_X, x_down_ref, 0, len(PLUS_X)),
    ):
        found = face(pl.ds(layer * rows_y, rows_y), members, x_in, first)
        for index, m in enumerate(members):
            out[index] = found[index]
            if m in DIAGONAL:
                row = rows_y - 1 if VELOCITY_TABLE[m][1] == 1 else 0
                corners[m][...] = found[index][row : row + 1]
    for members, out, row, first in (
        (PLUS_Y, y_up_ref, rows_y - 1, 0),
        (MINUS_Y, y_down_ref, 0, len(PLUS_Y)),
    ):
        def strided(ref, lanes):
            return jnp.concatenate(
                [ref[x * rows_y + row : x * rows_y + row + 1, lanes] for x in range(rows_x)], axis=0
            )

        velocity = [strided(moved_ref, slice(n * depth, (n + 1) * depth)) for n in range(3)]
        density = strided(density_ref, slice(0, depth))
        common = common_of(velocity)
        for index, m in enumerate(members):
            out[index] = relax(m, y_in[first + index], density, velocity, common)


def roll(value, steps, axis):
    if steps == 0:
        return value
    return pltpu.roll(value, steps % value.shape[axis], axis)


def collide_kernel(layers, pops_ref, velocity_ref, density_ref, out_ref, stage, sems):
    layer = pl.program_id(0)
    slot = lax.rem(layer, 2)
    depth = density_ref.shape[1]

    def each(which, at, action):
        for m in range(Q):
            step = VELOCITY_TABLE[m][0]

            def go(m=m, step=step):
                copy = pltpu.make_async_copy(stage.at[at, m], out_ref.at[m, which + step], sems.at[at, m])
                copy.start() if action == "start" else copy.wait()

            if step == 0:
                go()
            elif step == 1:
                pl.when(which < layers - 1)(go)
            else:
                pl.when(which > 0)(go)

    @pl.when(layer >= 2)
    def _():
        each(layer - 2, slot, "wait")

    velocity = [velocity_ref[:, n * depth : (n + 1) * depth] for n in range(3)]
    density = density_ref[...]
    common = common_of(velocity)
    for m in range(Q):
        value = relax(m, pops_ref[m, 0], density, velocity, common)
        value = roll(roll(value, VELOCITY_TABLE[m][1], 0), VELOCITY_TABLE[m][2], 1)
        stage[slot, m] = value
    each(layer, slot, "start")

    @pl.when(layer == layers - 1)
    def _():
        each(layer - 1, 1 - slot, "wait")
        each(layer, slot, "wait")


def edge_kernel(whole_ref, x_low, x_high, y_low, y_high, ca, cb, cc, cd, out_ref, face, strip, face_sem, strip_sem):
    del whole_ref
    layers, rows_y = out_ref.shape[1], out_ref.shape[2]
    corners = {7: ca, 8: cb, 9: cc, 10: cd}
    copies = []
    number = 0
    for members, source, layer in ((PLUS_X, x_low, 0), (MINUS_X, x_high, layers - 1)):
        for index, m in enumerate(members):
            step_y, step_z = VELOCITY_TABLE[m][1], VELOCITY_TABLE[m][2]
            value = source[index]
            if step_y == 1:
                value = jnp.concatenate([corners[m][...], value[: rows_y - 1]], axis=0)
            elif step_y == -1:
                value = jnp.concatenate([value[1:], corners[m][...]], axis=0)
            face[number] = roll(value, step_z, 1)
            copies.append(pltpu.make_async_copy(face.at[number], out_ref.at[m, layer], face_sem.at[number]))
            number += 1
    number = 0
    for members, source, row in ((PLUS_Y, y_low, 0), (MINUS_Y, y_high, rows_y - 1)):
        for index, m in enumerate(members):
            step_x, step_z = VELOCITY_TABLE[m][0], VELOCITY_TABLE[m][2]
            strip[number] = roll(source[index], step_z, 1)
            count = layers - abs(step_x)
            source_at = 1 if step_x == -1 else 0
            target_at = 1 if step_x == 1 else 0
            copies.append(
                pltpu.make_async_copy(
                    strip.at[number, pl.ds(source_at, count)],
                    out_ref.at[m, pl.ds(target_at, count), row],
                    strip_sem.at[number],
                )
            )
            number += 1
    for copy in copies:
        copy.start()
    for copy in copies:
        copy.wait()


def shifted(value, steps_x, steps_y):
    count_x, count_y = lax.axis_size("gx"), lax.axis_size("gy")
    pairs = []
    for x in range(count_x):
        for y in range(count_y):
            target = ((x + steps_x) % count_x) * count_y + (y + steps_y) % count_y
            pairs.append((x * count_y + y, target))
    return lax.ppermute(value, ("gx", "gy"), pairs)


def local(
    populations, rotation_init, slot_cell, slot_count, marker_arm, marker_area, marker_fraction
):
    _, size_x, size_y, depth = populations.shape
    slots = marker_area.shape[2]
    planes = size_x * size_y
    shape = jax.ShapeDtypeStruct
    params = pltpu.CompilerParams(vmem_limit_bytes=VMEM_LIMIT)
    cell = slot_cell.reshape(3, slots)
    plane = (cell[0] - lax.axis_index("gx") * size_x) * size_y + cell[1] - lax.axis_index("gy") * size_y
    active = lax.broadcasted_iota(jnp.int32, (slots,), 0) < slot_count.reshape(())
    weight = jnp.where(active, marker_area.reshape(-1), 0.0)
    pack = jnp.concatenate(
        [
            plane.astype(F32)[None],
            cell[2].astype(F32)[None],
            weight[None],
            marker_fraction.reshape(1, slots),
            marker_arm.reshape(3, slots),
            jnp.zeros((1, slots), F32),
        ],
        axis=0,
    )
    density, velocity = pl.pallas_call(
        moments_kernel,
        grid=(size_x,),
        in_specs=[pl.BlockSpec((Q, 1, size_y, depth), lambda x: (0, x, 0, 0))],
        out_specs=[
            pl.BlockSpec((size_y, depth), lambda x: (x, 0)),
            pl.BlockSpec((size_y, 3 * depth), lambda x: (x, 0)),
        ],
        out_shape=[shape((planes, depth), F32), shape((planes, 3 * depth), F32)],
        name="moments",
    )(populations)
    table = VMEM((slots // 256, slots, 256), BF16)
    sums, linear = pl.pallas_call(
        gather_kernel,
        in_specs=[vmem()] * 2,
        out_specs=[vmem()] * 2,
        out_shape=[shape((40, 128), F32), shape((16, slots), F32)],
        scratch_shapes=[
            VMEM((3 * depth, planes), BF16),
            VMEM((3 * depth, planes), BF16),
            VMEM((8, slots), F32),
            VMEM((8, slots), F32),
            VMEM((slots, 128), F32),
            VMEM((slots, 128), F32),
            table,
            table,
            table,
            VMEM((48, slots), BF16),
        ],
        compiler_params=params,
        name="gather",
    )(velocity, pack)
    count_x, count_y = lax.axis_size("gx"), lax.axis_size("gy")
    dma = pltpu.SemaphoreType.DMA
    sums = pl.pallas_call(
        functools.partial(total_kernel, count_x, count_y),
        in_specs=[vmem()],
        out_specs=vmem(),
        out_shape=shape((40, 128), F32),
        scratch_shapes=[
            VMEM((count_y - 1, 40, 128), F32),
            VMEM((40, 128), F32),
            VMEM((count_x - 1, 40, 128), F32),
            dma((count_y - 1,)),
            dma((count_y - 1,)),
            dma((count_x - 1,)),
            dma((count_x - 1,)),
        ],
        compiler_params=pltpu.CompilerParams(collective_id=0, has_side_effects=True),
        name="total",
    )(sums)
    x_face = shape((len(PLUS_X), size_y, depth), F32)
    y_face = shape((len(PLUS_Y), size_x, depth), F32)
    corner = shape((1, depth), F32)
    moved, spins, x_up, x_down, y_up, y_down, c7, c8, c9, c10 = pl.pallas_call(
        functools.partial(spread_kernel, size_y),
        in_specs=[vmem()] * 6 + [pl.BlockSpec(memory_space=pl.ANY)],
        out_specs=[vmem()] * 10,
        out_shape=[
            shape((planes, 3 * depth), F32),
            shape((8, 128), F32),
            x_face,
            x_face,
            y_face,
            y_face,
            corner,
            corner,
            corner,
            corner,
        ],
        scratch_shapes=[
            VMEM((planes, slots), BF16),
            VMEM((depth, slots), BF16),
            VMEM((depth, slots), BF16),
            VMEM((2 * len(PLUS_X), size_y, depth), F32),
            VMEM((2 * len(PLUS_Y), size_x, depth), F32),
            dma((2 * len(PLUS_X),)),
            dma((2 * len(PLUS_Y),)),
        ],
        compiler_params=params,
        name="spread",
    )(rotation_init.reshape(1, 3), sums, linear, pack, velocity, density, populations)
    x_low = shifted(x_up, 1, 0)
    x_high = shifted(x_down, -1, 0)
    y_low = shifted(y_up, 0, 1)
    y_high = shifted(y_down, 0, -1)
    c7, c8 = shifted(c7, 1, 1), shifted(c8, -1, -1)
    c9, c10 = shifted(c9, 1, -1), shifted(c10, -1, 1)
    whole = pl.pallas_call(
        functools.partial(collide_kernel, size_x),
        grid=(size_x,),
        in_specs=[
            pl.BlockSpec((Q, 1, size_y, depth), lambda x: (0, x, 0, 0)),
            pl.BlockSpec((size_y, 3 * depth), lambda x: (x, 0)),
            pl.BlockSpec((size_y, depth), lambda x: (x, 0)),
        ],
        out_specs=pl.BlockSpec(memory_space=pl.ANY),
        out_shape=shape(populations.shape, F32),
        scratch_shapes=[VMEM((2, Q, size_y, depth), F32), dma((2, Q))],
        cost_estimate=pl.CostEstimate(flops=100_000_000, bytes_accessed=20_000_000, transcendentals=0),
        name="collide",
    )(populations, moved, density)
    whole = pl.pallas_call(
        edge_kernel,
        in_specs=[pl.BlockSpec(memory_space=pl.ANY)] + [vmem()] * 8,
        out_specs=pl.BlockSpec(memory_space=pl.ANY),
        out_shape=shape(populations.shape, F32),
        scratch_shapes=[
            VMEM((2 * len(PLUS_X), size_y, depth), F32),
            VMEM((2 * len(PLUS_Y), size_x, depth), F32),
            dma((2 * len(PLUS_X),)),
            dma((2 * len(PLUS_Y),)),
        ],
        input_output_aliases={0: 0},
        name="edges",
    )(whole, x_low, x_high, y_low, y_high, c7, c8, c9, c10)
    return whole, spins[:ITERS, :3]


def solution(mesh):
    return jax.shard_map(
        local,
        mesh=mesh,
        in_specs=(
            P(None, "gx", "gy", None),
            P(),
            P(None, "gx", "gy", None),
            P("gx", "gy"),
            P(None, "gx", "gy", None),
            P("gx", "gy", None),
            P("gx", "gy", None),
        ),
        out_specs=(P(None, "gx", "gy", None), P()),
        check_vma=False,
    )
```

```python
import functools

import jax
import jax.numpy as jnp
from jax import lax
from jax.experimental import pallas as pl
from jax.experimental.pallas import tpu as pltpu
from jax.sharding import PartitionSpec as P

Q = 19
ITERS = 3
VELOCITY_TABLE = (
    (0, 0, 0),
    (1, 0, 0),
    (-1, 0, 0),
    (0, 1, 0),
    (0, -1, 0),
    (0, 0, 1),
    (0, 0, -1),
    (1, 1, 0),
    (-1, -1, 0),
    (1, -1, 0),
    (-1, 1, 0),
    (1, 0, 1),
    (-1, 0, -1),
    (1, 0, -1),
    (-1, 0, 1),
    (0, 1, 1),
    (0, -1, -1),
    (0, 1, -1),
    (0, -1, 1),
)
WEIGHT_TABLE = (1.0 / 3.0,) + (1.0 / 18.0,) * 6 + (1.0 / 36.0,) * 12
RELAX_TIME = 0.8
SPREAD_GAIN = 0.25
SPIN_GAIN = 0.5
PLUS_X = [m for m in range(Q) if VELOCITY_TABLE[m][0] == 1]
MINUS_X = [m for m in range(Q) if VELOCITY_TABLE[m][0] == -1]
PLUS_Y = [m for m in range(Q) if VELOCITY_TABLE[m][1] == 1]
MINUS_Y = [m for m in range(Q) if VELOCITY_TABLE[m][1] == -1]
DIAGONAL = [m for m in range(Q) if VELOCITY_TABLE[m][0] != 0 and VELOCITY_TABLE[m][1] != 0]
MESH = pl.DeviceIdType.MESH
F32 = jnp.float32
BF16 = jnp.bfloat16
VMEM = pltpu.VMEM
VMEM_LIMIT = 60 * 1024 * 1024


def vmem():
    return pl.BlockSpec(memory_space=pltpu.VMEM)


def relax(member, value, density, velocity, common):
    direction = VELOCITY_TABLE[member]
    projected = None
    for number in range(3):
        if direction[number] != 0:
            term = velocity[number] if direction[number] > 0 else -velocity[number]
            projected = term if projected is None else projected + term
    scaled = density * (WEIGHT_TABLE[member] / RELAX_TIME)
    if projected is None:
        bracket = common
    else:
        bracket = common + projected * (3.0 + 4.5 * projected)
    return value * (1.0 - 1.0 / RELAX_TIME) + scaled * bracket


def common_of(velocity):
    squared = velocity[0] * velocity[0] + velocity[1] * velocity[1] + velocity[2] * velocity[2]
    return 1.0 - 1.5 * squared


def moments_kernel(pops_ref, density_ref, velocity_ref, held, sems):
    layers, size_y, depth = pops_ref.shape[1], pops_ref.shape[2], pops_ref.shape[3]

    def incoming(layer):
        return pltpu.make_async_copy(pops_ref.at[:, layer], held.at[layer], sems.at[layer])

    for layer in range(layers):
        incoming(layer).start()

    def one(layer, carry):
        incoming(layer).wait()
        at = pl.ds(pl.multiple_of(layer * size_y, size_y), size_y)
        values = [held[layer, m] for m in range(Q)]
        density = values[0]
        for m in range(1, Q):
            density = density + values[m]
        density_ref[at, :] = density
        for number in range(3):
            total = None
            for m in range(Q):
                direction = VELOCITY_TABLE[m][number]
                if direction != 0:
                    if total is None:
                        total = values[m]
                    else:
                        total = total + values[m] if direction > 0 else total - values[m]
            velocity_ref[at, number * depth : (number + 1) * depth] = total / density
        return carry

    lax.fori_loop(0, layers, one, 0)


def pieces_of(value, count):
    found = []
    for number in range(count):
        piece = value.astype(BF16)
        found.append(piece)
        if number < count - 1:
            value = value - piece.astype(F32)
    return found


def depth_table(depth, low, fraction):
    high = jnp.where(low == depth - 1.0, 0.0, low + 1.0)
    ids = lax.broadcasted_iota(jnp.int32, (depth, low.shape[1]), 0).astype(F32)
    return jnp.where(ids == low, 1.0 - fraction, 0.0) + jnp.where(ids == high, fraction, 0.0)


def plane_table(planes, row):
    ids = lax.broadcasted_iota(jnp.int32, (planes, row.shape[1]), 0).astype(F32)
    return jnp.where(ids == row, 1.0, 0.0).astype(BF16)


def gather_kernel(
    velocity_ref,
    pack_ref,
    sums_ref,
    linear_ref,
    turned_hi,
    turned_lo,
    state_ref,
    result_ref,
    cell_col,
    high_col,
    same_ref,
    after_ref,
    before_ref,
    left_ref,
):
    planes, triple = velocity_ref.shape
    depth = triple // 3
    slots = pack_ref.shape[1]
    turned = jnp.transpose(velocity_ref[...])
    hi, lo = pieces_of(turned, 2)
    turned_hi[...] = hi
    turned_lo[...] = lo
    chunk = 256
    steps = slots // chunk

    def gather(step, carry):
        at = pl.ds(pl.multiple_of(step * chunk, chunk), chunk)
        table = plane_table(planes, pack_ref[0:1, at])
        rows = jnp.dot(turned_hi[...], table, preferred_element_type=F32)
        rows = rows + jnp.dot(turned_lo[...], table, preferred_element_type=F32)
        tap = depth_table(depth, pack_ref[1:2, at], pack_ref[3:4, at])
        for number in range(3):
            part = rows[number * depth : (number + 1) * depth]
            state_ref[number : number + 1, at] = jnp.sum(part * tap, axis=0, keepdims=True)
        return carry

    lax.fori_loop(0, steps, gather, 0)
    state_ref[3:6, :] = pack_ref[4:7, :]
    state_ref[6:8, :] = jnp.zeros((2, slots), F32)

    low = pack_ref[1:2, :]
    high = jnp.where(low == depth - 1.0, 0.0, low + 1.0)
    base = pack_ref[0:1, :] * float(depth)
    cell_row = base + low
    high_row = base + high
    both = jnp.concatenate([cell_row, high_row, jnp.zeros((6, slots), F32)], axis=0)
    columns = jnp.transpose(both)
    cell_col[...] = jnp.broadcast_to(columns[:, 0:1], (slots, 128))
    high_col[...] = jnp.broadcast_to(columns[:, 1:2], (slots, 128))
    result_ref[6:8, :] = both[0:2]

    def prepare():
        weighted = state_ref[...] * pack_ref[2:3, :]
        share = pack_ref[3:4, :]
        stacked = jnp.concatenate([weighted * (1.0 - share), weighted * share], axis=0)
        left_ref[...] = jnp.concatenate(pieces_of(stacked, 3), axis=0)

    def apply(build):
        def one(step, carry):
            at = pl.ds(pl.multiple_of(step * chunk, chunk), chunk)
            if build:
                for half in range(chunk // 128):
                    part = pl.ds(pl.multiple_of(step * chunk + half * 128, 128), 128)
                    lanes = slice(half * 128, (half + 1) * 128)
                    cell = result_ref[6:7, part]
                    cell_high = result_ref[7:8, part]
                    same_ref[step, :, lanes] = jnp.where(cell_col[...] == cell, 1.0, 0.0).astype(BF16)
                    after_ref[step, :, lanes] = jnp.where(high_col[...] == cell, 1.0, 0.0).astype(BF16)
                    before_ref[step, :, lanes] = jnp.where(cell_col[...] == cell_high, 1.0, 0.0).astype(BF16)
            left = left_ref[...]

            def product(table):
                out = jnp.dot(left, table, preferred_element_type=F32)
                return out[0:16] + out[16:32] + out[32:48]

            same = product(same_ref[step])
            after = product(after_ref[step])
            before = product(before_ref[step])
            share = pack_ref[3:4, at]
            total = (1.0 - share) * (same[0:8] + after[8:16]) + share * (same[8:16] + before[0:8])
            result_ref[0:6, at] = SPREAD_GAIN * total[0:6]
            return carry

        lax.fori_loop(0, steps, one, 0)

    prepare()
    apply(True)
    arm = pack_ref[4:7, :]
    weight = pack_ref[2:3, :]
    first = state_ref[0:3, :]
    second = first - result_ref[0:3, :]
    carried = result_ref[3:6, :]
    state_ref[0:3, :] = second
    state_ref[3:6, :] = carried
    prepare()
    apply(False)
    third = second - result_ref[0:3, :]
    later = carried - result_ref[3:6, :]
    heavy = arm * weight
    rows = []
    for vector in (arm, carried, later):
        for a in range(3):
            rows.append(heavy[a : a + 1] * vector)
    for vector in (first, second, third):
        rows.append(heavy[1:2] * vector[2:3] - heavy[2:3] * vector[1:2])
        rows.append(heavy[2:3] * vector[0:1] - heavy[0:1] * vector[2:3])
        rows.append(heavy[0:1] * vector[1:2] - heavy[1:2] * vector[0:1])
    rows.append(jnp.zeros((4, slots), F32))
    table = jnp.concatenate(rows, axis=0)
    column = jnp.broadcast_to(jnp.sum(table, axis=1, keepdims=True), (40, 128))
    square = jnp.concatenate([column, jnp.zeros((88, 128), F32)], axis=0)
    sums_ref[...] = jnp.transpose(square)[0:8]
    linear_ref[0:3, :] = heavy
    linear_ref[3:6, :] = weight * (first + second + third)
    linear_ref[6:9, :] = weight * (carried + later)
    linear_ref[9:12, :] = weight * carried
    linear_ref[12:16, :] = jnp.zeros((4, slots), F32)


def total_kernel(x_count, y_count, part_ref, out_ref, near, mine, far, near_send, near_recv, far_send, far_recv):
    x = lax.axis_index("gx")
    y = lax.axis_index("gy")
    barrier = pltpu.get_barrier_semaphore()
    for step in range(1, y_count):
        pl.semaphore_signal(barrier, inc=1, device_id=(x, lax.rem(y + step, y_count)), device_id_type=MESH)
    for step in range(1, x_count):
        pl.semaphore_signal(barrier, inc=1, device_id=(lax.rem(x + step, x_count), y), device_id_type=MESH)
    pl.semaphore_wait(barrier, x_count + y_count - 2)

    def near_copy(step):
        return pltpu.make_async_remote_copy(
            src_ref=part_ref,
            dst_ref=near.at[step - 1],
            send_sem=near_send.at[step - 1],
            recv_sem=near_recv.at[step - 1],
            device_id=(x, lax.rem(y + step, y_count)),
            device_id_type=MESH,
        )

    def far_copy(step):
        return pltpu.make_async_remote_copy(
            src_ref=mine,
            dst_ref=far.at[step - 1],
            send_sem=far_send.at[step - 1],
            recv_sem=far_recv.at[step - 1],
            device_id=(lax.rem(x + step, x_count), y),
            device_id_type=MESH,
        )

    def ordered(own, slots, count, position):
        total = None
        for source in range(count):
            value = own
            for step in range(1, count):
                hit = lax.rem(position + count - step, count) == source
                value = jnp.where(hit, slots[step - 1], value)
            total = value if total is None else total + value
        return total

    for step in range(1, y_count):
        near_copy(step).start()
    for step in range(1, y_count):
        near_copy(step).wait()
    mine[...] = ordered(part_ref[...], near, y_count, y)
    for step in range(1, x_count):
        far_copy(step).start()
    for step in range(1, x_count):
        far_copy(step).wait()
    out_ref[...] = ordered(mine[...], far, x_count, x)


def cross(first, second):
    return [
        first[1] * second[2] - first[2] * second[1],
        first[2] * second[0] - first[0] * second[2],
        first[0] * second[1] - first[1] * second[0],
    ]


def spread_kernel(
    rows_y,
    spin_ref,
    sums_ref,
    linear_ref,
    pack_ref,
    velocity_ref,
    density_ref,
    pops_ref,
    moved_ref,
    spins_ref,
    x_up_ref,
    x_down_ref,
    y_up_ref,
    y_down_ref,
    corner_a,
    corner_b,
    corner_c,
    corner_d,
    table_ref,
    hi_ref,
    lo_ref,
    x_in,
    y_in,
    turned,
    x_sem,
    y_sem,
):
    planes, depth = density_ref.shape
    rows_x = planes // rows_y
    copies = []
    for number, m in enumerate(PLUS_X + MINUS_X):
        layer = rows_x - 1 if m in PLUS_X else 0
        copies.append(pltpu.make_async_copy(pops_ref.at[m, layer], x_in.at[number], x_sem.at[number]))
    for number, m in enumerate(PLUS_Y + MINUS_Y):
        row = rows_y - 1 if m in PLUS_Y else 0
        copies.append(pltpu.make_async_copy(pops_ref.at[m, :, row], y_in.at[number], y_sem.at[number]))
    for copy in copies:
        copy.start()

    turned[...] = jnp.transpose(jnp.broadcast_to(sums_ref[0:1, :], (128, 128)))

    def number_at(index):
        return turned[index : index + 1, 0:1]

    def turning(offset, spin):
        entry = [[number_at(offset + a * 3 + b) for b in range(3)] for a in range(3)]
        trace = entry[0][0] + entry[1][1] + entry[2][2]
        return [
            spin[b] * trace - (entry[0][b] * spin[0] + entry[1][b] * spin[1] + entry[2][b] * spin[2])
            for b in range(3)
        ]

    inertia = number_at(0) + number_at(4) + number_at(8)
    spin = [spin_ref[0:1, number : number + 1] for number in range(3)]
    spins = [spin]
    spins_ref[...] = jnp.zeros(spins_ref.shape, F32)
    for step in range(ITERS):
        own = turning(0, spins[step])
        torque = [number_at(27 + step * 3 + b) - own[b] for b in range(3)]
        if step >= 1:
            back = turning(9, spins[step - 1])
            torque = [torque[b] + back[b] for b in range(3)]
        if step >= 2:
            back = turning(18, spins[step - 2])
            torque = [torque[b] + back[b] for b in range(3)]
        spins.append([spins[step][b] + SPIN_GAIN * torque[b] / inertia for b in range(3)])
        for b in range(3):
            spins_ref[step : step + 1, b : b + 1] = spins[step + 1][b]
    whole = [spins[0][b] + spins[1][b] + spins[2][b] for b in range(3)]

    def linear(start):
        return [linear_ref[start + b : start + b + 1, :] for b in range(3)]

    lead = cross(whole, linear(0))
    fall = linear(3)
    zeroth = cross(spins[0], linear(6))
    once = cross(spins[1], linear(9))
    impulse = [SPREAD_GAIN * (lead[b] - fall[b] - zeroth[b] - once[b]) for b in range(3)]
    table_ref[...] = plane_table(planes, pack_ref[0:1, :])
    tap = depth_table(depth, pack_ref[1:2, :], pack_ref[3:4, :])
    for number in range(3):
        lanes = slice(number * depth, (number + 1) * depth)
        hi, lo = pieces_of(tap * impulse[number], 2)
        hi_ref[...] = hi
        lo_ref[...] = lo
        dims = (((1,), (1,)), ((), ()))
        added = lax.dot_general(table_ref[...], hi_ref[...], dims, preferred_element_type=F32)
        added = added + lax.dot_general(table_ref[...], lo_ref[...], dims, preferred_element_type=F32)
        moved_ref[:, lanes] = velocity_ref[:, lanes] + added

    for copy in copies:
        copy.wait()

    def face(at, members, incoming, first):
        velocity = [moved_ref[at, number * depth : (number + 1) * depth] for number in range(3)]
        common = common_of(velocity)
        density = density_ref[at, :]
        return [
            relax(m, incoming[first + index], density, velocity, common)
            for index, m in enumerate(members)
        ]

    corners = {7: corner_a, 8: corner_b, 9: corner_c, 10: corner_d}
    for members, out, layer, first in (
        (PLUS_X, x_up_ref, rows_x - 1, 0),
        (MINUS_X, x_down_ref, 0, len(PLUS_X)),
    ):
        found = face(pl.ds(layer * rows_y, rows_y), members, x_in, first)
        for index, m in enumerate(members):
            out[index] = found[index]
            if m in DIAGONAL:
                row = rows_y - 1 if VELOCITY_TABLE[m][1] == 1 else 0
                corners[m][...] = found[index][row : row + 1]
    for members, out, row, first in (
        (PLUS_Y, y_up_ref, rows_y - 1, 0),
        (MINUS_Y, y_down_ref, 0, len(PLUS_Y)),
    ):
        def strided(ref, lanes):
            return jnp.concatenate(
                [ref[x * rows_y + row : x * rows_y + row + 1, lanes] for x in range(rows_x)], axis=0
            )

        velocity = [strided(moved_ref, slice(n * depth, (n + 1) * depth)) for n in range(3)]
        density = strided(density_ref, slice(0, depth))
        common = common_of(velocity)
        for index, m in enumerate(members):
            out[index] = relax(m, y_in[first + index], density, velocity, common)


def roll(value, steps, axis):
    if steps == 0:
        return value
    return pltpu.roll(value, steps % value.shape[axis], axis)


def collide_kernel(layers, pops_ref, velocity_ref, density_ref, out_ref, held, speed, mass, in_sems, sems):
    size_y, depth = held.shape[2], held.shape[3]

    def incoming(layer):
        rows = pl.ds(pl.multiple_of(layer * size_y, size_y), size_y)
        return [
            pltpu.make_async_copy(pops_ref.at[:, layer], held.at[layer], in_sems.at[0, layer]),
            pltpu.make_async_copy(velocity_ref.at[rows], speed.at[layer], in_sems.at[1, layer]),
            pltpu.make_async_copy(density_ref.at[rows], mass.at[layer], in_sems.at[2, layer]),
        ]

    def outgoing(layer, action):
        for m in range(Q):
            step = VELOCITY_TABLE[m][0]

            def go(m=m, step=step):
                copy = pltpu.make_async_copy(held.at[layer, m], out_ref.at[m, layer + step], sems.at[layer, m])
                copy.start() if action == "start" else copy.wait()

            if step == 0:
                go()
            elif step == 1:
                pl.when(layer < layers - 1)(go)
            else:
                pl.when(layer > 0)(go)

    for layer in range(layers):
        for copy in incoming(layer):
            copy.start()

    def one(layer, carry):
        for copy in incoming(layer):
            copy.wait()
        velocity = [speed[layer, :, n * depth : (n + 1) * depth] for n in range(3)]
        density = mass[layer]
        common = common_of(velocity)
        for m in range(Q):
            value = relax(m, held[layer, m], density, velocity, common)
            value = roll(roll(value, VELOCITY_TABLE[m][1], 0), VELOCITY_TABLE[m][2], 1)
            held[layer, m] = value
        outgoing(layer, "start")
        return carry

    lax.fori_loop(0, layers, one, 0)

    def finish(layer, carry):
        outgoing(layer, "wait")
        return carry

    lax.fori_loop(0, layers, finish, 0)


def trade_kernel(x_count, y_count, *refs):
    ways = ((0, 1), (0, -1), (1, 1), (-1, -1), (1, -1), (-1, 1))
    count = len(ways)
    sources, targets, slots = refs[:count], refs[count : 2 * count], refs[2 * count : 3 * count]
    send_sem, recv_sem = refs[3 * count :]
    x = lax.axis_index("gx")
    y = lax.axis_index("gy")
    others = [(lax.rem(x + dx + x_count, x_count), lax.rem(y + dy + y_count, y_count)) for dx, dy in ways]
    barrier = pltpu.get_barrier_semaphore()
    for other in others:
        pl.semaphore_signal(barrier, inc=1, device_id=other, device_id_type=MESH)
    pl.semaphore_wait(barrier, count)
    copies = [
        pltpu.make_async_remote_copy(
            src_ref=sources[n],
            dst_ref=slots[n],
            send_sem=send_sem.at[n],
            recv_sem=recv_sem.at[n],
            device_id=others[n],
            device_id_type=MESH,
        )
        for n in range(count)
    ]
    for copy in copies:
        copy.start()
    for copy in copies:
        copy.wait()
    for n in range(count):
        targets[n][...] = slots[n][...]


def edge_kernel(whole_ref, x_low, x_high, y_low, y_high, ca, cb, cc, cd, out_ref, face, strip, face_sem, strip_sem):
    del whole_ref
    layers, rows_y = out_ref.shape[1], out_ref.shape[2]
    corners = {7: ca, 8: cb, 9: cc, 10: cd}
    copies = []
    number = 0
    for members, source, layer in ((PLUS_X, x_low, 0), (MINUS_X, x_high, layers - 1)):
        for index, m in enumerate(members):
            step_y, step_z = VELOCITY_TABLE[m][1], VELOCITY_TABLE[m][2]
            value = source[index]
            if step_y == 1:
                value = jnp.concatenate([corners[m][...], value[: rows_y - 1]], axis=0)
            elif step_y == -1:
                value = jnp.concatenate([value[1:], corners[m][...]], axis=0)
            face[number] = roll(value, step_z, 1)
            copies.append(pltpu.make_async_copy(face.at[number], out_ref.at[m, layer], face_sem.at[number]))
            number += 1
    number = 0
    for members, source, row in ((PLUS_Y, y_low, 0), (MINUS_Y, y_high, rows_y - 1)):
        for index, m in enumerate(members):
            step_x, step_z = VELOCITY_TABLE[m][0], VELOCITY_TABLE[m][2]
            strip[number] = roll(source[index], step_z, 1)
            count = layers - abs(step_x)
            source_at = 1 if step_x == -1 else 0
            target_at = 1 if step_x == 1 else 0
            copies.append(
                pltpu.make_async_copy(
                    strip.at[number, pl.ds(source_at, count)],
                    out_ref.at[m, pl.ds(target_at, count), row],
                    strip_sem.at[number],
                )
            )
            number += 1
    for copy in copies:
        copy.start()
    for copy in copies:
        copy.wait()


def shifted(value, steps_x, steps_y):
    count_x, count_y = lax.axis_size("gx"), lax.axis_size("gy")
    pairs = []
    for x in range(count_x):
        for y in range(count_y):
            target = ((x + steps_x) % count_x) * count_y + (y + steps_y) % count_y
            pairs.append((x * count_y + y, target))
    return lax.ppermute(value, ("gx", "gy"), pairs)


def local(
    populations, rotation_init, slot_cell, slot_count, marker_arm, marker_area, marker_fraction
):
    _, size_x, size_y, depth = populations.shape
    slots = marker_area.shape[2]
    planes = size_x * size_y
    shape = jax.ShapeDtypeStruct
    params = pltpu.CompilerParams(vmem_limit_bytes=VMEM_LIMIT)
    cell = slot_cell.reshape(3, slots)
    plane = (cell[0] - lax.axis_index("gx") * size_x) * size_y + cell[1] - lax.axis_index("gy") * size_y
    active = lax.broadcasted_iota(jnp.int32, (slots,), 0) < slot_count.reshape(())
    weight = jnp.where(active, marker_area.reshape(-1), 0.0)
    pack = jnp.concatenate(
        [
            plane.astype(F32)[None],
            cell[2].astype(F32)[None],
            weight[None],
            marker_fraction.reshape(1, slots),
            marker_arm.reshape(3, slots),
            jnp.zeros((1, slots), F32),
        ],
        axis=0,
    )
    held = VMEM((size_x, Q, size_y, depth), F32)
    density, velocity = pl.pallas_call(
        moments_kernel,
        in_specs=[pl.BlockSpec(memory_space=pl.ANY)],
        out_specs=[vmem(), vmem()],
        out_shape=[shape((planes, depth), F32), shape((planes, 3 * depth), F32)],
        scratch_shapes=[held, pltpu.SemaphoreType.DMA((size_x,))],
        compiler_params=params,
        name="moments",
    )(populations)
    table = VMEM((slots // 256, slots, 256), BF16)
    sums, linear = pl.pallas_call(
        gather_kernel,
        in_specs=[vmem()] * 2,
        out_specs=[vmem()] * 2,
        out_shape=[shape((8, 128), F32), shape((16, slots), F32)],
        scratch_shapes=[
            VMEM((3 * depth, planes), BF16),
            VMEM((3 * depth, planes), BF16),
            VMEM((8, slots), F32),
            VMEM((8, slots), F32),
            VMEM((slots, 128), F32),
            VMEM((slots, 128), F32),
            table,
            table,
            table,
            VMEM((48, slots), BF16),
        ],
        compiler_params=params,
        name="gather",
    )(velocity, pack)
    count_x, count_y = lax.axis_size("gx"), lax.axis_size("gy")
    dma = pltpu.SemaphoreType.DMA
    sums = pl.pallas_call(
        functools.partial(total_kernel, count_x, count_y),
        in_specs=[vmem()],
        out_specs=vmem(),
        out_shape=shape((8, 128), F32),
        scratch_shapes=[
            VMEM((count_y - 1, 8, 128), F32),
            VMEM((8, 128), F32),
            VMEM((count_x - 1, 8, 128), F32),
            dma((count_y - 1,)),
            dma((count_y - 1,)),
            dma((count_x - 1,)),
            dma((count_x - 1,)),
        ],
        compiler_params=pltpu.CompilerParams(collective_id=0, has_side_effects=True),
        name="total",
    )(sums)
    x_face = shape((len(PLUS_X), size_y, depth), F32)
    y_face = shape((len(PLUS_Y), size_x, depth), F32)
    corner = shape((1, depth), F32)
    moved, spins, x_up, x_down, y_up, y_down, c7, c8, c9, c10 = pl.pallas_call(
        functools.partial(spread_kernel, size_y),
        in_specs=[vmem()] * 6 + [pl.BlockSpec(memory_space=pl.ANY)],
        out_specs=[vmem()] * 10,
        out_shape=[
            shape((planes, 3 * depth), F32),
            shape((8, 128), F32),
            x_face,
            x_face,
            y_face,
            y_face,
            corner,
            corner,
            corner,
            corner,
        ],
        scratch_shapes=[
            VMEM((planes, slots), BF16),
            VMEM((depth, slots), BF16),
            VMEM((depth, slots), BF16),
            VMEM((2 * len(PLUS_X), size_y, depth), F32),
            VMEM((2 * len(PLUS_Y), size_x, depth), F32),
            VMEM((128, 128), F32),
            dma((2 * len(PLUS_X),)),
            dma((2 * len(PLUS_Y),)),
        ],
        compiler_params=params,
        name="spread",
    )(rotation_init.reshape(1, 3), sums, linear, pack, velocity, density, populations)
    x_low = shifted(x_up, 1, 0)
    x_high = shifted(x_down, -1, 0)
    small = [y_face, y_face, corner, corner, corner, corner]
    y_low, y_high, c7, c8, c9, c10 = pl.pallas_call(
        functools.partial(trade_kernel, count_x, count_y),
        in_specs=[vmem()] * 6,
        out_specs=[vmem()] * 6,
        out_shape=small,
        scratch_shapes=[VMEM(one.shape, F32) for one in small] + [dma((6,)), dma((6,))],
        compiler_params=pltpu.CompilerParams(collective_id=1, has_side_effects=True),
        cost_estimate=pl.CostEstimate(flops=20_000_000, bytes_accessed=1_000_000, transcendentals=0),
        name="trade",
    )(y_up, y_down, c7, c8, c9, c10)
    whole = pl.pallas_call(
        functools.partial(collide_kernel, size_x),
        in_specs=[pl.BlockSpec(memory_space=pl.ANY)] * 3,
        out_specs=pl.BlockSpec(memory_space=pl.ANY),
        out_shape=shape(populations.shape, F32),
        scratch_shapes=[
            held,
            VMEM((size_x, size_y, 3 * depth), F32),
            VMEM((size_x, size_y, depth), F32),
            dma((3, size_x)),
            dma((size_x, Q)),
        ],
        compiler_params=params,
        cost_estimate=pl.CostEstimate(flops=100_000_000, bytes_accessed=20_000_000, transcendentals=0),
        name="collide",
    )(populations, moved, density)
    whole = pl.pallas_call(
        edge_kernel,
        in_specs=[pl.BlockSpec(memory_space=pl.ANY)] + [vmem()] * 8,
        out_specs=pl.BlockSpec(memory_space=pl.ANY),
        out_shape=shape(populations.shape, F32),
        scratch_shapes=[
            VMEM((2 * len(PLUS_X), size_y, depth), F32),
            VMEM((2 * len(PLUS_Y), size_x, depth), F32),
            dma((2 * len(PLUS_X),)),
            dma((2 * len(PLUS_Y),)),
        ],
        input_output_aliases={0: 0},
        name="edges",
    )(whole, x_low, x_high, y_low, y_high, c7, c8, c9, c10)
    return whole, spins[:ITERS, :3]


def solution(mesh):
    return jax.shard_map(
        local,
        mesh=mesh,
        in_specs=(
            P(None, "gx", "gy", None),
            P(),
            P(None, "gx", "gy", None),
            P("gx", "gy"),
            P(None, "gx", "gy", None),
            P("gx", "gy", None),
            P("gx", "gy", None),
        ),
        out_specs=(P(None, "gx", "gy", None), P()),
        check_vma=False,
    )
```

```python
import functools

import jax
import jax.numpy as jnp
from jax import lax
from jax.experimental import pallas as pl
from jax.experimental.pallas import tpu as pltpu
from jax.sharding import PartitionSpec as P

Q = 19
ITERS = 3
VELOCITY_TABLE = (
    (0, 0, 0),
    (1, 0, 0),
    (-1, 0, 0),
    (0, 1, 0),
    (0, -1, 0),
    (0, 0, 1),
    (0, 0, -1),
    (1, 1, 0),
    (-1, -1, 0),
    (1, -1, 0),
    (-1, 1, 0),
    (1, 0, 1),
    (-1, 0, -1),
    (1, 0, -1),
    (-1, 0, 1),
    (0, 1, 1),
    (0, -1, -1),
    (0, 1, -1),
    (0, -1, 1),
)
WEIGHT_TABLE = (1.0 / 3.0,) + (1.0 / 18.0,) * 6 + (1.0 / 36.0,) * 12
RELAX_TIME = 0.8
SPREAD_GAIN = 0.25
SPIN_GAIN = 0.5
PLUS_X = [m for m in range(Q) if VELOCITY_TABLE[m][0] == 1]
MINUS_X = [m for m in range(Q) if VELOCITY_TABLE[m][0] == -1]
PLUS_Y = [m for m in range(Q) if VELOCITY_TABLE[m][1] == 1]
MINUS_Y = [m for m in range(Q) if VELOCITY_TABLE[m][1] == -1]
DIAGONAL = [m for m in range(Q) if VELOCITY_TABLE[m][0] != 0 and VELOCITY_TABLE[m][1] != 0]
MESH = pl.DeviceIdType.MESH
F32 = jnp.float32
BF16 = jnp.bfloat16
VMEM = pltpu.VMEM
VMEM_LIMIT = 60 * 1024 * 1024


def vmem():
    return pl.BlockSpec(memory_space=pltpu.VMEM)


def relax(member, value, density, velocity, common):
    direction = VELOCITY_TABLE[member]
    projected = None
    for number in range(3):
        if direction[number] != 0:
            term = velocity[number] if direction[number] > 0 else -velocity[number]
            projected = term if projected is None else projected + term
    scaled = density * (WEIGHT_TABLE[member] / RELAX_TIME)
    if projected is None:
        bracket = common
    else:
        bracket = common + projected * (3.0 + 4.5 * projected)
    return value * (1.0 - 1.0 / RELAX_TIME) + scaled * bracket


def common_of(velocity):
    squared = velocity[0] * velocity[0] + velocity[1] * velocity[1] + velocity[2] * velocity[2]
    return 1.0 - 1.5 * squared


def moments_kernel(pops_ref, density_ref, velocity_ref, held, sems):
    layers, size_y, depth = pops_ref.shape[1], pops_ref.shape[2], pops_ref.shape[3]

    def incoming(layer):
        return pltpu.make_async_copy(pops_ref.at[:, layer], held.at[layer], sems.at[layer])

    for layer in range(layers):
        incoming(layer).start()

    def one(layer, carry):
        incoming(layer).wait()
        at = pl.ds(pl.multiple_of(layer * size_y, size_y), size_y)
        values = [held[layer, m] for m in range(Q)]
        density = values[0]
        for m in range(1, Q):
            density = density + values[m]
        density_ref[at, :] = density
        for number in range(3):
            total = None
            for m in range(Q):
                direction = VELOCITY_TABLE[m][number]
                if direction != 0:
                    if total is None:
                        total = values[m]
                    else:
                        total = total + values[m] if direction > 0 else total - values[m]
            velocity_ref[at, number * depth : (number + 1) * depth] = total / density
        return carry

    lax.fori_loop(0, layers, one, 0)


def pieces_of(value, count):
    found = []
    for number in range(count):
        piece = value.astype(BF16)
        found.append(piece)
        if number < count - 1:
            value = value - piece.astype(F32)
    return found


def depth_table(depth, low, fraction):
    high = jnp.where(low == depth - 1.0, 0.0, low + 1.0)
    ids = lax.broadcasted_iota(jnp.int32, (depth, low.shape[1]), 0).astype(F32)
    return jnp.where(ids == low, 1.0 - fraction, 0.0) + jnp.where(ids == high, fraction, 0.0)


def plane_table(planes, row):
    ids = lax.broadcasted_iota(jnp.int32, (planes, row.shape[1]), 0).astype(F32)
    return jnp.where(ids == row, 1.0, 0.0).astype(BF16)


def gather_kernel(
    velocity_ref,
    pack_ref,
    sums_ref,
    linear_ref,
    turned_hi,
    turned_lo,
    state_ref,
    result_ref,
    cell_col,
    high_col,
    same_ref,
    after_ref,
    before_ref,
    left_ref,
):
    planes, triple = velocity_ref.shape
    depth = triple // 3
    slots = pack_ref.shape[1]
    turned = jnp.transpose(velocity_ref[...])
    hi, lo = pieces_of(turned, 2)
    turned_hi[...] = hi
    turned_lo[...] = lo
    chunk = 512
    steps = slots // chunk

    def gather(step, carry):
        at = pl.ds(pl.multiple_of(step * chunk, chunk), chunk)
        table = plane_table(planes, pack_ref[0:1, at])
        rows = jnp.dot(turned_hi[...], table, preferred_element_type=F32)
        rows = rows + jnp.dot(turned_lo[...], table, preferred_element_type=F32)
        tap = depth_table(depth, pack_ref[1:2, at], pack_ref[3:4, at])
        for number in range(3):
            part = rows[number * depth : (number + 1) * depth]
            state_ref[number : number + 1, at] = jnp.sum(part * tap, axis=0, keepdims=True)
        return carry

    lax.fori_loop(0, steps, gather, 0)
    state_ref[3:6, :] = pack_ref[4:7, :]
    state_ref[6:8, :] = jnp.zeros((2, slots), F32)

    low = pack_ref[1:2, :]
    high = jnp.where(low == depth - 1.0, 0.0, low + 1.0)
    base = pack_ref[0:1, :] * float(depth)
    cell_row = base + low
    high_row = base + high
    both = jnp.concatenate([cell_row, high_row, jnp.zeros((6, slots), F32)], axis=0)
    columns = jnp.transpose(both)
    cell_col[...] = jnp.broadcast_to(columns[:, 0:1], (slots, 128))
    high_col[...] = jnp.broadcast_to(columns[:, 1:2], (slots, 128))
    result_ref[6:8, :] = both[0:2]

    def prepare():
        weighted = state_ref[...] * pack_ref[2:3, :]
        share = pack_ref[3:4, :]
        stacked = jnp.concatenate([weighted * (1.0 - share), weighted * share], axis=0)
        left_ref[...] = jnp.concatenate(pieces_of(stacked, 3), axis=0)

    def apply(build):
        def one(step, carry):
            at = pl.ds(pl.multiple_of(step * chunk, chunk), chunk)
            if build:
                for half in range(chunk // 128):
                    part = pl.ds(pl.multiple_of(step * chunk + half * 128, 128), 128)
                    lanes = slice(half * 128, (half + 1) * 128)
                    cell = result_ref[6:7, part]
                    cell_high = result_ref[7:8, part]
                    same_ref[step, :, lanes] = jnp.where(cell_col[...] == cell, 1.0, 0.0).astype(BF16)
                    after_ref[step, :, lanes] = jnp.where(high_col[...] == cell, 1.0, 0.0).astype(BF16)
                    before_ref[step, :, lanes] = jnp.where(cell_col[...] == cell_high, 1.0, 0.0).astype(BF16)
            left = left_ref[...]

            def product(table):
                out = jnp.dot(left, table, preferred_element_type=F32)
                return out[0:16] + out[16:32] + out[32:48]

            same = product(same_ref[step])
            after = product(after_ref[step])
            before = product(before_ref[step])
            share = pack_ref[3:4, at]
            total = (1.0 - share) * (same[0:8] + after[8:16]) + share * (same[8:16] + before[0:8])
            result_ref[0:6, at] = SPREAD_GAIN * total[0:6]
            return carry

        lax.fori_loop(0, steps, one, 0)

    prepare()
    apply(True)
    arm = pack_ref[4:7, :]
    weight = pack_ref[2:3, :]
    first = state_ref[0:3, :]
    second = first - result_ref[0:3, :]
    carried = result_ref[3:6, :]
    state_ref[0:3, :] = second
    state_ref[3:6, :] = carried
    prepare()
    apply(False)
    third = second - result_ref[0:3, :]
    later = carried - result_ref[3:6, :]
    heavy = arm * weight
    rows = []
    for vector in (arm, carried, later):
        for a in range(3):
            rows.append(heavy[a : a + 1] * vector)
    for vector in (first, second, third):
        rows.append(heavy[1:2] * vector[2:3] - heavy[2:3] * vector[1:2])
        rows.append(heavy[2:3] * vector[0:1] - heavy[0:1] * vector[2:3])
        rows.append(heavy[0:1] * vector[1:2] - heavy[1:2] * vector[0:1])
    rows.append(jnp.zeros((4, slots), F32))
    table = jnp.concatenate(rows, axis=0)
    column = jnp.broadcast_to(jnp.sum(table, axis=1, keepdims=True), (40, 128))
    square = jnp.concatenate([column, jnp.zeros((88, 128), F32)], axis=0)
    sums_ref[...] = jnp.transpose(square)[0:8]
    linear_ref[0:3, :] = heavy
    linear_ref[3:6, :] = weight * (first + second + third)
    linear_ref[6:9, :] = weight * (carried + later)
    linear_ref[9:12, :] = weight * carried
    linear_ref[12:16, :] = jnp.zeros((4, slots), F32)


def total_kernel(x_count, y_count, part_ref, out_ref, near, mine, far, near_send, near_recv, far_send, far_recv):
    x = lax.axis_index("gx")
    y = lax.axis_index("gy")
    barrier = pltpu.get_barrier_semaphore()
    for step in range(1, y_count):
        pl.semaphore_signal(barrier, inc=1, device_id=(x, lax.rem(y + step, y_count)), device_id_type=MESH)
    for step in range(1, x_count):
        pl.semaphore_signal(barrier, inc=1, device_id=(lax.rem(x + step, x_count), y), device_id_type=MESH)
    pl.semaphore_wait(barrier, x_count + y_count - 2)

    def near_copy(step):
        return pltpu.make_async_remote_copy(
            src_ref=part_ref,
            dst_ref=near.at[step - 1],
            send_sem=near_send.at[step - 1],
            recv_sem=near_recv.at[step - 1],
            device_id=(x, lax.rem(y + step, y_count)),
            device_id_type=MESH,
        )

    def far_copy(step):
        return pltpu.make_async_remote_copy(
            src_ref=mine,
            dst_ref=far.at[step - 1],
            send_sem=far_send.at[step - 1],
            recv_sem=far_recv.at[step - 1],
            device_id=(lax.rem(x + step, x_count), y),
            device_id_type=MESH,
        )

    def ordered(own, slots, count, position):
        total = None
        for source in range(count):
            value = own
            for step in range(1, count):
                hit = lax.rem(position + count - step, count) == source
                value = jnp.where(hit, slots[step - 1], value)
            total = value if total is None else total + value
        return total

    for step in range(1, y_count):
        near_copy(step).start()
    for step in range(1, y_count):
        near_copy(step).wait()
    mine[...] = ordered(part_ref[...], near, y_count, y)
    for step in range(1, x_count):
        far_copy(step).start()
    for step in range(1, x_count):
        far_copy(step).wait()
    out_ref[...] = ordered(mine[...], far, x_count, x)


def cross(first, second):
    return [
        first[1] * second[2] - first[2] * second[1],
        first[2] * second[0] - first[0] * second[2],
        first[0] * second[1] - first[1] * second[0],
    ]


def spread_kernel(
    rows_y,
    spin_ref,
    sums_ref,
    linear_ref,
    pack_ref,
    velocity_ref,
    density_ref,
    pops_ref,
    moved_ref,
    spins_ref,
    x_up_ref,
    x_down_ref,
    y_up_ref,
    y_down_ref,
    corner_a,
    corner_b,
    corner_c,
    corner_d,
    table_ref,
    hi_ref,
    lo_ref,
    x_in,
    y_in,
    turned,
    x_sem,
    y_sem,
):
    planes, depth = density_ref.shape
    rows_x = planes // rows_y
    copies = []
    for number, m in enumerate(PLUS_X + MINUS_X):
        layer = rows_x - 1 if m in PLUS_X else 0
        copies.append(pltpu.make_async_copy(pops_ref.at[m, layer], x_in.at[number], x_sem.at[number]))
    for number, m in enumerate(PLUS_Y + MINUS_Y):
        row = rows_y - 1 if m in PLUS_Y else 0
        copies.append(pltpu.make_async_copy(pops_ref.at[m, :, row], y_in.at[number], y_sem.at[number]))
    for copy in copies:
        copy.start()

    turned[...] = jnp.transpose(jnp.broadcast_to(sums_ref[0:1, :], (128, 128)))

    def number_at(index):
        return turned[index : index + 1, 0:1]

    def turning(offset, spin):
        entry = [[number_at(offset + a * 3 + b) for b in range(3)] for a in range(3)]
        trace = entry[0][0] + entry[1][1] + entry[2][2]
        return [
            spin[b] * trace - (entry[0][b] * spin[0] + entry[1][b] * spin[1] + entry[2][b] * spin[2])
            for b in range(3)
        ]

    inertia = number_at(0) + number_at(4) + number_at(8)
    spin = [spin_ref[0:1, number : number + 1] for number in range(3)]
    spins = [spin]
    spins_ref[...] = jnp.zeros(spins_ref.shape, F32)
    for step in range(ITERS):
        own = turning(0, spins[step])
        torque = [number_at(27 + step * 3 + b) - own[b] for b in range(3)]
        if step >= 1:
            back = turning(9, spins[step - 1])
            torque = [torque[b] + back[b] for b in range(3)]
        if step >= 2:
            back = turning(18, spins[step - 2])
            torque = [torque[b] + back[b] for b in range(3)]
        spins.append([spins[step][b] + SPIN_GAIN * torque[b] / inertia for b in range(3)])
        for b in range(3):
            spins_ref[step : step + 1, b : b + 1] = spins[step + 1][b]
    whole = [spins[0][b] + spins[1][b] + spins[2][b] for b in range(3)]

    def linear(start):
        return [linear_ref[start + b : start + b + 1, :] for b in range(3)]

    lead = cross(whole, linear(0))
    fall = linear(3)
    zeroth = cross(spins[0], linear(6))
    once = cross(spins[1], linear(9))
    impulse = [SPREAD_GAIN * (lead[b] - fall[b] - zeroth[b] - once[b]) for b in range(3)]
    table_ref[...] = plane_table(planes, pack_ref[0:1, :])
    tap = depth_table(depth, pack_ref[1:2, :], pack_ref[3:4, :])
    for number in range(3):
        lanes = slice(number * depth, (number + 1) * depth)
        hi, lo = pieces_of(tap * impulse[number], 2)
        hi_ref[lanes, :] = hi
        lo_ref[lanes, :] = lo
    dims = (((1,), (1,)), ((), ()))
    added = lax.dot_general(table_ref[...], hi_ref[...], dims, preferred_element_type=F32)
    added = added + lax.dot_general(table_ref[...], lo_ref[...], dims, preferred_element_type=F32)
    moved_ref[...] = velocity_ref[...] + added

    for copy in copies:
        copy.wait()

    def face(at, members, incoming, first):
        velocity = [moved_ref[at, number * depth : (number + 1) * depth] for number in range(3)]
        common = common_of(velocity)
        density = density_ref[at, :]
        return [
            relax(m, incoming[first + index], density, velocity, common)
            for index, m in enumerate(members)
        ]

    corners = {7: corner_a, 8: corner_b, 9: corner_c, 10: corner_d}
    for members, out, layer, first in (
        (PLUS_X, x_up_ref, rows_x - 1, 0),
        (MINUS_X, x_down_ref, 0, len(PLUS_X)),
    ):
        found = face(pl.ds(layer * rows_y, rows_y), members, x_in, first)
        for index, m in enumerate(members):
            out[index] = found[index]
            if m in DIAGONAL:
                row = rows_y - 1 if VELOCITY_TABLE[m][1] == 1 else 0
                corners[m][...] = found[index][row : row + 1]
    for members, out, row, first in (
        (PLUS_Y, y_up_ref, rows_y - 1, 0),
        (MINUS_Y, y_down_ref, 0, len(PLUS_Y)),
    ):
        def strided(ref, lanes):
            return jnp.concatenate(
                [ref[x * rows_y + row : x * rows_y + row + 1, lanes] for x in range(rows_x)], axis=0
            )

        velocity = [strided(moved_ref, slice(n * depth, (n + 1) * depth)) for n in range(3)]
        density = strided(density_ref, slice(0, depth))
        common = common_of(velocity)
        for index, m in enumerate(members):
            out[index] = relax(m, y_in[first + index], density, velocity, common)


def roll(value, steps, axis):
    if steps == 0:
        return value
    return pltpu.roll(value, steps % value.shape[axis], axis)


def collide_kernel(layers, pops_ref, velocity_ref, density_ref, out_ref, held, speed, mass, in_sems, sems):
    size_y, depth = held.shape[2], held.shape[3]

    def incoming(layer):
        rows = pl.ds(pl.multiple_of(layer * size_y, size_y), size_y)
        return [
            pltpu.make_async_copy(pops_ref.at[:, layer], held.at[layer], in_sems.at[0, layer]),
            pltpu.make_async_copy(velocity_ref.at[rows], speed.at[layer], in_sems.at[1, layer]),
            pltpu.make_async_copy(density_ref.at[rows], mass.at[layer], in_sems.at[2, layer]),
        ]

    def outgoing(layer, action):
        for m in range(Q):
            step = VELOCITY_TABLE[m][0]

            def go(m=m, step=step):
                copy = pltpu.make_async_copy(held.at[layer, m], out_ref.at[m, layer + step], sems.at[layer, m])
                copy.start() if action == "start" else copy.wait()

            if step == 0:
                go()
            elif step == 1:
                pl.when(layer < layers - 1)(go)
            else:
                pl.when(layer > 0)(go)

    for layer in range(layers):
        for copy in incoming(layer):
            copy.start()

    def one(layer, carry):
        for copy in incoming(layer):
            copy.wait()
        velocity = [speed[layer, :, n * depth : (n + 1) * depth] for n in range(3)]
        density = mass[layer]
        common = common_of(velocity)
        for m in range(Q):
            value = relax(m, held[layer, m], density, velocity, common)
            value = roll(roll(value, VELOCITY_TABLE[m][1], 0), VELOCITY_TABLE[m][2], 1)
            held[layer, m] = value
        outgoing(layer, "start")
        return carry

    lax.fori_loop(0, layers, one, 0)

    def finish(layer, carry):
        outgoing(layer, "wait")
        return carry

    lax.fori_loop(0, layers, finish, 0)


def trade_kernel(x_count, y_count, *refs):
    ways = ((0, 1), (0, -1), (1, 1), (-1, -1), (1, -1), (-1, 1))
    count = len(ways)
    sources = refs[:count]
    targets, slots = refs[count + 1 : 2 * count + 1], refs[2 * count + 1 : 3 * count + 1]
    send_sem, recv_sem = refs[3 * count + 1 :]
    x = lax.axis_index("gx")
    y = lax.axis_index("gy")
    others = [(lax.rem(x + dx + x_count, x_count), lax.rem(y + dy + y_count, y_count)) for dx, dy in ways]
    barrier = pltpu.get_barrier_semaphore()
    for other in others:
        pl.semaphore_signal(barrier, inc=1, device_id=other, device_id_type=MESH)
    pl.semaphore_wait(barrier, count)
    copies = [
        pltpu.make_async_remote_copy(
            src_ref=sources[n],
            dst_ref=slots[n],
            send_sem=send_sem.at[n],
            recv_sem=recv_sem.at[n],
            device_id=others[n],
            device_id_type=MESH,
        )
        for n in range(count)
    ]
    for copy in copies:
        copy.start()
    for copy in copies:
        copy.wait()
    for n in range(count):
        targets[n][...] = slots[n][...]


def edge_kernel(whole_ref, x_low, x_high, y_low, y_high, ca, cb, cc, cd, out_ref, face, strip, face_sem, strip_sem):
    del whole_ref
    layers, rows_y = out_ref.shape[1], out_ref.shape[2]
    corners = {7: ca, 8: cb, 9: cc, 10: cd}
    copies = []
    number = 0
    for members, source, layer in ((PLUS_X, x_low, 0), (MINUS_X, x_high, layers - 1)):
        for index, m in enumerate(members):
            step_y, step_z = VELOCITY_TABLE[m][1], VELOCITY_TABLE[m][2]
            value = source[index]
            if step_y == 1:
                value = jnp.concatenate([corners[m][...], value[: rows_y - 1]], axis=0)
            elif step_y == -1:
                value = jnp.concatenate([value[1:], corners[m][...]], axis=0)
            face[number] = roll(value, step_z, 1)
            copies.append(pltpu.make_async_copy(face.at[number], out_ref.at[m, layer], face_sem.at[number]))
            number += 1
    number = 0
    for members, source, row in ((PLUS_Y, y_low, 0), (MINUS_Y, y_high, rows_y - 1)):
        for index, m in enumerate(members):
            step_x, step_z = VELOCITY_TABLE[m][0], VELOCITY_TABLE[m][2]
            strip[number] = roll(source[index], step_z, 1)
            count = layers - abs(step_x)
            source_at = 1 if step_x == -1 else 0
            target_at = 1 if step_x == 1 else 0
            copies.append(
                pltpu.make_async_copy(
                    strip.at[number, pl.ds(source_at, count)],
                    out_ref.at[m, pl.ds(target_at, count), row],
                    strip_sem.at[number],
                )
            )
            number += 1
    for copy in copies:
        copy.start()
    for copy in copies:
        copy.wait()


def shifted(value, steps_x, steps_y):
    count_x, count_y = lax.axis_size("gx"), lax.axis_size("gy")
    pairs = []
    for x in range(count_x):
        for y in range(count_y):
            target = ((x + steps_x) % count_x) * count_y + (y + steps_y) % count_y
            pairs.append((x * count_y + y, target))
    return lax.ppermute(value, ("gx", "gy"), pairs)


def local(
    populations, rotation_init, slot_cell, slot_count, marker_arm, marker_area, marker_fraction
):
    _, size_x, size_y, depth = populations.shape
    slots = marker_area.shape[2]
    planes = size_x * size_y
    shape = jax.ShapeDtypeStruct
    params = pltpu.CompilerParams(vmem_limit_bytes=VMEM_LIMIT)
    cell = slot_cell.reshape(3, slots)
    plane = (cell[0] - lax.axis_index("gx") * size_x) * size_y + cell[1] - lax.axis_index("gy") * size_y
    active = lax.broadcasted_iota(jnp.int32, (slots,), 0) < slot_count.reshape(())
    weight = jnp.where(active, marker_area.reshape(-1), 0.0)
    pack = jnp.concatenate(
        [
            plane.astype(F32)[None],
            cell[2].astype(F32)[None],
            weight[None],
            marker_fraction.reshape(1, slots),
            marker_arm.reshape(3, slots),
            jnp.zeros((1, slots), F32),
        ],
        axis=0,
    )
    held = VMEM((size_x, Q, size_y, depth), F32)
    density, velocity = pl.pallas_call(
        moments_kernel,
        in_specs=[pl.BlockSpec(memory_space=pl.ANY)],
        out_specs=[vmem(), vmem()],
        out_shape=[shape((planes, depth), F32), shape((planes, 3 * depth), F32)],
        scratch_shapes=[held, pltpu.SemaphoreType.DMA((size_x,))],
        compiler_params=params,
        name="moments",
    )(populations)
    table = VMEM((slots // 512, slots, 512), BF16)
    sums, linear = pl.pallas_call(
        gather_kernel,
        in_specs=[vmem()] * 2,
        out_specs=[vmem()] * 2,
        out_shape=[shape((8, 128), F32), shape((16, slots), F32)],
        scratch_shapes=[
            VMEM((3 * depth, planes), BF16),
            VMEM((3 * depth, planes), BF16),
            VMEM((8, slots), F32),
            VMEM((8, slots), F32),
            VMEM((slots, 128), F32),
            VMEM((slots, 128), F32),
            table,
            table,
            table,
            VMEM((48, slots), BF16),
        ],
        compiler_params=params,
        name="gather",
    )(velocity, pack)
    count_x, count_y = lax.axis_size("gx"), lax.axis_size("gy")
    dma = pltpu.SemaphoreType.DMA
    sums = pl.pallas_call(
        functools.partial(total_kernel, count_x, count_y),
        in_specs=[vmem()],
        out_specs=vmem(),
        out_shape=shape((8, 128), F32),
        scratch_shapes=[
            VMEM((count_y - 1, 8, 128), F32),
            VMEM((8, 128), F32),
            VMEM((count_x - 1, 8, 128), F32),
            dma((count_y - 1,)),
            dma((count_y - 1,)),
            dma((count_x - 1,)),
            dma((count_x - 1,)),
        ],
        compiler_params=pltpu.CompilerParams(collective_id=0, has_side_effects=True),
        name="total",
    )(sums)
    x_face = shape((len(PLUS_X), size_y, depth), F32)
    y_face = shape((len(PLUS_Y), size_x, depth), F32)
    corner = shape((1, depth), F32)
    moved, spins, x_up, x_down, y_up, y_down, c7, c8, c9, c10 = pl.pallas_call(
        functools.partial(spread_kernel, size_y),
        in_specs=[vmem()] * 6 + [pl.BlockSpec(memory_space=pl.ANY)],
        out_specs=[vmem()] * 10,
        out_shape=[
            shape((planes, 3 * depth), F32),
            shape((8, 128), F32),
            x_face,
            x_face,
            y_face,
            y_face,
            corner,
            corner,
            corner,
            corner,
        ],
        scratch_shapes=[
            VMEM((planes, slots), BF16),
            VMEM((3 * depth, slots), BF16),
            VMEM((3 * depth, slots), BF16),
            VMEM((2 * len(PLUS_X), size_y, depth), F32),
            VMEM((2 * len(PLUS_Y), size_x, depth), F32),
            VMEM((128, 128), F32),
            dma((2 * len(PLUS_X),)),
            dma((2 * len(PLUS_Y),)),
        ],
        compiler_params=params,
        name="spread",
    )(rotation_init.reshape(1, 3), sums, linear, pack, velocity, density, populations)
    x_low = shifted(x_up, 1, 0)
    x_high = shifted(x_down, -1, 0)
    whole = pl.pallas_call(
        functools.partial(collide_kernel, size_x),
        in_specs=[pl.BlockSpec(memory_space=pl.ANY)] * 3,
        out_specs=pl.BlockSpec(memory_space=pl.ANY),
        out_shape=shape(populations.shape, F32),
        scratch_shapes=[
            held,
            VMEM((size_x, size_y, 3 * depth), F32),
            VMEM((size_x, size_y, depth), F32),
            dma((3, size_x)),
            dma((size_x, Q)),
        ],
        compiler_params=params,
        cost_estimate=pl.CostEstimate(flops=100_000_000, bytes_accessed=20_000_000, transcendentals=0),
        name="collide",
    )(populations, moved, density)
    small = [y_face, y_face, corner, corner, corner, corner]
    y_low, y_high, c7, c8, c9, c10 = pl.pallas_call(
        functools.partial(trade_kernel, count_x, count_y),
        in_specs=[vmem()] * 6 + [pl.BlockSpec(memory_space=pl.ANY)],
        out_specs=[vmem()] * 6,
        out_shape=small,
        scratch_shapes=[VMEM(one.shape, F32) for one in small] + [dma((6,)), dma((6,))],
        compiler_params=pltpu.CompilerParams(collective_id=1, has_side_effects=True),
        cost_estimate=pl.CostEstimate(flops=20_000_000, bytes_accessed=1_000_000, transcendentals=0),
        name="trade",
    )(y_up, y_down, c7, c8, c9, c10, whole)
    whole = pl.pallas_call(
        edge_kernel,
        in_specs=[pl.BlockSpec(memory_space=pl.ANY)] + [vmem()] * 8,
        out_specs=pl.BlockSpec(memory_space=pl.ANY),
        out_shape=shape(populations.shape, F32),
        scratch_shapes=[
            VMEM((2 * len(PLUS_X), size_y, depth), F32),
            VMEM((2 * len(PLUS_Y), size_x, depth), F32),
            dma((2 * len(PLUS_X),)),
            dma((2 * len(PLUS_Y),)),
        ],
        input_output_aliases={0: 0},
        name="edges",
    )(whole, x_low, x_high, y_low, y_high, c7, c8, c9, c10)
    return whole, spins[:ITERS, :3]


def solution(mesh):
    return jax.shard_map(
        local,
        mesh=mesh,
        in_specs=(
            P(None, "gx", "gy", None),
            P(),
            P(None, "gx", "gy", None),
            P("gx", "gy"),
            P(None, "gx", "gy", None),
            P("gx", "gy", None),
            P("gx", "gy", None),
        ),
        out_specs=(P(None, "gx", "gy", None), P()),
        check_vma=False,
    )
```

```python
import functools

import jax
import jax.numpy as jnp
from jax import lax
from jax.experimental import pallas as pl
from jax.experimental.pallas import tpu as pltpu
from jax.sharding import PartitionSpec as P

Q = 19
ITERS = 3
VELOCITY_TABLE = (
    (0, 0, 0),
    (1, 0, 0),
    (-1, 0, 0),
    (0, 1, 0),
    (0, -1, 0),
    (0, 0, 1),
    (0, 0, -1),
    (1, 1, 0),
    (-1, -1, 0),
    (1, -1, 0),
    (-1, 1, 0),
    (1, 0, 1),
    (-1, 0, -1),
    (1, 0, -1),
    (-1, 0, 1),
    (0, 1, 1),
    (0, -1, -1),
    (0, 1, -1),
    (0, -1, 1),
)
WEIGHT_TABLE = (1.0 / 3.0,) + (1.0 / 18.0,) * 6 + (1.0 / 36.0,) * 12
RELAX_TIME = 0.8
SPREAD_GAIN = 0.25
SPIN_GAIN = 0.5
PLUS_X = [m for m in range(Q) if VELOCITY_TABLE[m][0] == 1]
MINUS_X = [m for m in range(Q) if VELOCITY_TABLE[m][0] == -1]
PLUS_Y = [m for m in range(Q) if VELOCITY_TABLE[m][1] == 1]
MINUS_Y = [m for m in range(Q) if VELOCITY_TABLE[m][1] == -1]
DIAGONAL = [m for m in range(Q) if VELOCITY_TABLE[m][0] != 0 and VELOCITY_TABLE[m][1] != 0]
MESH = pl.DeviceIdType.MESH
F32 = jnp.float32
BF16 = jnp.bfloat16
VMEM = pltpu.VMEM
VMEM_LIMIT = 60 * 1024 * 1024


def vmem():
    return pl.BlockSpec(memory_space=pltpu.VMEM)


def relax(member, value, density, velocity, common):
    direction = VELOCITY_TABLE[member]
    projected = None
    for number in range(3):
        if direction[number] != 0:
            term = velocity[number] if direction[number] > 0 else -velocity[number]
            projected = term if projected is None else projected + term
    scaled = density * (WEIGHT_TABLE[member] / RELAX_TIME)
    if projected is None:
        bracket = common
    else:
        bracket = common + projected * (3.0 + 4.5 * projected)
    return value * (1.0 - 1.0 / RELAX_TIME) + scaled * bracket


def common_of(velocity):
    squared = velocity[0] * velocity[0] + velocity[1] * velocity[1] + velocity[2] * velocity[2]
    return 1.0 - 1.5 * squared


def moments_kernel(pops_ref, density_ref, velocity_ref, held, sems):
    layers, size_y, depth = pops_ref.shape[1], pops_ref.shape[2], pops_ref.shape[3]

    def incoming(layer):
        return pltpu.make_async_copy(pops_ref.at[:, layer], held.at[layer], sems.at[layer])

    for layer in range(layers):
        incoming(layer).start()

    def one(layer, carry):
        incoming(layer).wait()
        at = pl.ds(pl.multiple_of(layer * size_y, size_y), size_y)
        values = [held[layer, m] for m in range(Q)]
        density = values[0]
        for m in range(1, Q):
            density = density + values[m]
        density_ref[at, :] = density
        for number in range(3):
            total = None
            for m in range(Q):
                direction = VELOCITY_TABLE[m][number]
                if direction != 0:
                    if total is None:
                        total = values[m]
                    else:
                        total = total + values[m] if direction > 0 else total - values[m]
            velocity_ref[at, number * depth : (number + 1) * depth] = total / density
        return carry

    lax.fori_loop(0, layers, one, 0)


def pieces_of(value, count):
    found = []
    for number in range(count):
        piece = value.astype(BF16)
        found.append(piece)
        if number < count - 1:
            value = value - piece.astype(F32)
    return found


def depth_table(depth, low, fraction):
    high = jnp.where(low == depth - 1.0, 0.0, low + 1.0)
    ids = lax.broadcasted_iota(jnp.int32, (depth, low.shape[1]), 0).astype(F32)
    return jnp.where(ids == low, 1.0 - fraction, 0.0) + jnp.where(ids == high, fraction, 0.0)


def plane_table(planes, row):
    ids = lax.broadcasted_iota(jnp.int32, (planes, row.shape[1]), 0).astype(F32)
    return jnp.where(ids == row, 1.0, 0.0).astype(BF16)


def gather_kernel(
    velocity_ref,
    pack_ref,
    sums_ref,
    linear_ref,
    turned_hi,
    turned_lo,
    state_ref,
    result_ref,
    cell_col,
    high_col,
    same_ref,
    after_ref,
    before_ref,
    left_ref,
):
    planes, triple = velocity_ref.shape
    depth = triple // 3
    slots = pack_ref.shape[1]
    turned = jnp.transpose(velocity_ref[...])
    hi, lo = pieces_of(turned, 2)
    turned_hi[...] = hi
    turned_lo[...] = lo
    chunk = 512
    steps = slots // chunk

    def gather(step, carry):
        at = pl.ds(pl.multiple_of(step * chunk, chunk), chunk)
        table = plane_table(planes, pack_ref[0:1, at])
        rows = jnp.dot(turned_hi[...], table, preferred_element_type=F32)
        rows = rows + jnp.dot(turned_lo[...], table, preferred_element_type=F32)
        tap = depth_table(depth, pack_ref[1:2, at], pack_ref[3:4, at])
        for number in range(3):
            part = rows[number * depth : (number + 1) * depth]
            state_ref[number : number + 1, at] = jnp.sum(part * tap, axis=0, keepdims=True)
        return carry

    lax.fori_loop(0, steps, gather, 0)
    state_ref[3:6, :] = pack_ref[4:7, :]
    state_ref[6:8, :] = jnp.zeros((2, slots), F32)

    low = pack_ref[1:2, :]
    high = jnp.where(low == depth - 1.0, 0.0, low + 1.0)
    base = pack_ref[0:1, :] * float(depth)
    cell_row = base + low
    high_row = base + high
    both = jnp.concatenate([cell_row, high_row, jnp.zeros((6, slots), F32)], axis=0)
    columns = jnp.transpose(both)
    cell_col[...] = jnp.broadcast_to(columns[:, 0:1], (slots, 128))
    high_col[...] = jnp.broadcast_to(columns[:, 1:2], (slots, 128))
    result_ref[6:8, :] = both[0:2]

    def prepare():
        weighted = state_ref[...] * pack_ref[2:3, :]
        share = pack_ref[3:4, :]
        stacked = jnp.concatenate([weighted * (1.0 - share), weighted * share], axis=0)
        left_ref[...] = jnp.concatenate(pieces_of(stacked, 3), axis=0)

    def apply(build):
        def one(step, carry):
            at = pl.ds(pl.multiple_of(step * chunk, chunk), chunk)
            if build:
                for half in range(chunk // 128):
                    part = pl.ds(pl.multiple_of(step * chunk + half * 128, 128), 128)
                    lanes = slice(half * 128, (half + 1) * 128)
                    cell = result_ref[6:7, part]
                    cell_high = result_ref[7:8, part]
                    same_ref[step, :, lanes] = jnp.where(cell_col[...] == cell, 1.0, 0.0).astype(BF16)
                    after_ref[step, :, lanes] = jnp.where(high_col[...] == cell, 1.0, 0.0).astype(BF16)
                    before_ref[step, :, lanes] = jnp.where(cell_col[...] == cell_high, 1.0, 0.0).astype(BF16)
            left = left_ref[...]

            def product(table):
                out = jnp.dot(left, table, preferred_element_type=F32)
                return out[0:16] + out[16:32] + out[32:48]

            same = product(same_ref[step])
            after = product(after_ref[step])
            before = product(before_ref[step])
            share = pack_ref[3:4, at]
            total = (1.0 - share) * (same[0:8] + after[8:16]) + share * (same[8:16] + before[0:8])
            result_ref[0:6, at] = SPREAD_GAIN * total[0:6]
            return carry

        lax.fori_loop(0, steps, one, 0)

    prepare()
    apply(True)
    arm = pack_ref[4:7, :]
    weight = pack_ref[2:3, :]
    first = state_ref[0:3, :]
    second = first - result_ref[0:3, :]
    carried = result_ref[3:6, :]
    state_ref[0:3, :] = second
    state_ref[3:6, :] = carried
    prepare()
    apply(False)
    third = second - result_ref[0:3, :]
    later = carried - result_ref[3:6, :]
    heavy = arm * weight
    rows = []
    for vector in (arm, carried, later):
        for a in range(3):
            rows.append(heavy[a : a + 1] * vector)
    for vector in (first, second, third):
        rows.append(heavy[1:2] * vector[2:3] - heavy[2:3] * vector[1:2])
        rows.append(heavy[2:3] * vector[0:1] - heavy[0:1] * vector[2:3])
        rows.append(heavy[0:1] * vector[1:2] - heavy[1:2] * vector[0:1])
    rows.append(jnp.zeros((4, slots), F32))
    table = jnp.concatenate(rows, axis=0)
    column = jnp.broadcast_to(jnp.sum(table, axis=1, keepdims=True), (40, 128))
    square = jnp.concatenate([column, jnp.zeros((88, 128), F32)], axis=0)
    sums_ref[...] = jnp.transpose(square)[0:8]
    linear_ref[0:3, :] = heavy
    linear_ref[3:6, :] = weight * (first + second + third)
    linear_ref[6:9, :] = weight * (carried + later)
    linear_ref[9:12, :] = weight * carried
    linear_ref[12:16, :] = jnp.zeros((4, slots), F32)


def total_kernel(x_count, y_count, part_ref, out_ref, near, mine, far, near_send, near_recv, far_send, far_recv):
    x = lax.axis_index("gx")
    y = lax.axis_index("gy")
    barrier = pltpu.get_barrier_semaphore()
    for step in range(1, y_count):
        pl.semaphore_signal(barrier, inc=1, device_id=(x, lax.rem(y + step, y_count)), device_id_type=MESH)
    for step in range(1, x_count):
        pl.semaphore_signal(barrier, inc=1, device_id=(lax.rem(x + step, x_count), y), device_id_type=MESH)
    pl.semaphore_wait(barrier, x_count + y_count - 2)

    def near_copy(step):
        return pltpu.make_async_remote_copy(
            src_ref=part_ref,
            dst_ref=near.at[step - 1],
            send_sem=near_send.at[step - 1],
            recv_sem=near_recv.at[step - 1],
            device_id=(x, lax.rem(y + step, y_count)),
            device_id_type=MESH,
        )

    def far_copy(step):
        return pltpu.make_async_remote_copy(
            src_ref=mine,
            dst_ref=far.at[step - 1],
            send_sem=far_send.at[step - 1],
            recv_sem=far_recv.at[step - 1],
            device_id=(lax.rem(x + step, x_count), y),
            device_id_type=MESH,
        )

    def ordered(own, slots, count, position):
        total = None
        for source in range(count):
            value = own
            for step in range(1, count):
                hit = lax.rem(position + count - step, count) == source
                value = jnp.where(hit, slots[step - 1], value)
            total = value if total is None else total + value
        return total

    for step in range(1, y_count):
        near_copy(step).start()
    for step in range(1, y_count):
        near_copy(step).wait()
    mine[...] = ordered(part_ref[...], near, y_count, y)
    for step in range(1, x_count):
        far_copy(step).start()
    for step in range(1, x_count):
        far_copy(step).wait()
    out_ref[...] = ordered(mine[...], far, x_count, x)


def cross(first, second):
    return [
        first[1] * second[2] - first[2] * second[1],
        first[2] * second[0] - first[0] * second[2],
        first[0] * second[1] - first[1] * second[0],
    ]


def spread_kernel(
    rows_y,
    spin_ref,
    sums_ref,
    linear_ref,
    pack_ref,
    velocity_ref,
    density_ref,
    pops_ref,
    moved_ref,
    spins_ref,
    x_up_ref,
    x_down_ref,
    y_up_ref,
    y_down_ref,
    corner_a,
    corner_b,
    corner_c,
    corner_d,
    table_ref,
    hi_ref,
    lo_ref,
    x_in,
    y_in,
    turned,
    x_sem,
    y_sem,
):
    planes, depth = density_ref.shape
    rows_x = planes // rows_y
    copies = []
    for number, m in enumerate(PLUS_X + MINUS_X):
        layer = rows_x - 1 if m in PLUS_X else 0
        copies.append(pltpu.make_async_copy(pops_ref.at[m, layer], x_in.at[number], x_sem.at[number]))
    for number, m in enumerate(PLUS_Y + MINUS_Y):
        row = rows_y - 1 if m in PLUS_Y else 0
        copies.append(pltpu.make_async_copy(pops_ref.at[m, :, row], y_in.at[number], y_sem.at[number]))
    for copy in copies:
        copy.start()

    turned[...] = jnp.transpose(jnp.broadcast_to(sums_ref[0:1, :], (128, 128)))

    def number_at(index):
        return turned[index : index + 1, 0:1]

    def turning(offset, spin):
        entry = [[number_at(offset + a * 3 + b) for b in range(3)] for a in range(3)]
        trace = entry[0][0] + entry[1][1] + entry[2][2]
        return [
            spin[b] * trace - (entry[0][b] * spin[0] + entry[1][b] * spin[1] + entry[2][b] * spin[2])
            for b in range(3)
        ]

    inertia = number_at(0) + number_at(4) + number_at(8)
    spin = [spin_ref[0:1, number : number + 1] for number in range(3)]
    spins = [spin]
    for step in range(ITERS):
        own = turning(0, spins[step])
        torque = [number_at(27 + step * 3 + b) - own[b] for b in range(3)]
        if step >= 1:
            back = turning(9, spins[step - 1])
            torque = [torque[b] + back[b] for b in range(3)]
        if step >= 2:
            back = turning(18, spins[step - 2])
            torque = [torque[b] + back[b] for b in range(3)]
        spins.append([spins[step][b] + SPIN_GAIN * torque[b] / inertia for b in range(3)])
        for b in range(3):
            spins_ref[step : step + 1, b : b + 1] = spins[step + 1][b]
    whole = [spins[0][b] + spins[1][b] + spins[2][b] for b in range(3)]

    def linear(start):
        return [linear_ref[start + b : start + b + 1, :] for b in range(3)]

    lead = cross(whole, linear(0))
    fall = linear(3)
    zeroth = cross(spins[0], linear(6))
    once = cross(spins[1], linear(9))
    impulse = [SPREAD_GAIN * (lead[b] - fall[b] - zeroth[b] - once[b]) for b in range(3)]
    table_ref[...] = plane_table(planes, pack_ref[0:1, :])
    tap = depth_table(depth, pack_ref[1:2, :], pack_ref[3:4, :])
    for number in range(3):
        lanes = slice(number * depth, (number + 1) * depth)
        hi, lo = pieces_of(tap * impulse[number], 2)
        hi_ref[lanes, :] = hi
        lo_ref[lanes, :] = lo
    dims = (((1,), (1,)), ((), ()))
    added = lax.dot_general(table_ref[...], hi_ref[...], dims, preferred_element_type=F32)
    added = added + lax.dot_general(table_ref[...], lo_ref[...], dims, preferred_element_type=F32)
    moved_ref[...] = velocity_ref[...] + added

    for copy in copies:
        copy.wait()

    def face(at, members, incoming, first):
        velocity = [moved_ref[at, number * depth : (number + 1) * depth] for number in range(3)]
        common = common_of(velocity)
        density = density_ref[at, :]
        return [
            relax(m, incoming[first + index], density, velocity, common)
            for index, m in enumerate(members)
        ]

    corners = {7: corner_a, 8: corner_b, 9: corner_c, 10: corner_d}
    for members, out, layer, first in (
        (PLUS_X, x_up_ref, rows_x - 1, 0),
        (MINUS_X, x_down_ref, 0, len(PLUS_X)),
    ):
        found = face(pl.ds(layer * rows_y, rows_y), members, x_in, first)
        for index, m in enumerate(members):
            out[index] = found[index]
            if m in DIAGONAL:
                row = rows_y - 1 if VELOCITY_TABLE[m][1] == 1 else 0
                corners[m][...] = found[index][row : row + 1]
    for members, out, row, first in (
        (PLUS_Y, y_up_ref, rows_y - 1, 0),
        (MINUS_Y, y_down_ref, 0, len(PLUS_Y)),
    ):
        def strided(ref, lanes):
            return jnp.concatenate(
                [ref[x * rows_y + row : x * rows_y + row + 1, lanes] for x in range(rows_x)], axis=0
            )

        velocity = [strided(moved_ref, slice(n * depth, (n + 1) * depth)) for n in range(3)]
        density = strided(density_ref, slice(0, depth))
        common = common_of(velocity)
        for index, m in enumerate(members):
            out[index] = relax(m, y_in[first + index], density, velocity, common)


def roll(value, steps, axis):
    if steps == 0:
        return value
    return pltpu.roll(value, steps % value.shape[axis], axis)


def collide_kernel(layers, pops_ref, velocity_ref, density_ref, out_ref, held, speed, mass, in_sems, sems):
    size_y, depth = held.shape[2], held.shape[3]

    def incoming(layer):
        rows = pl.ds(pl.multiple_of(layer * size_y, size_y), size_y)
        return [
            pltpu.make_async_copy(pops_ref.at[:, layer], held.at[layer], in_sems.at[0, layer]),
            pltpu.make_async_copy(velocity_ref.at[rows], speed.at[layer], in_sems.at[1, layer]),
            pltpu.make_async_copy(density_ref.at[rows], mass.at[layer], in_sems.at[2, layer]),
        ]

    def outgoing(layer, action):
        for m in range(Q):
            step = VELOCITY_TABLE[m][0]

            def go(m=m, step=step):
                copy = pltpu.make_async_copy(held.at[layer, m], out_ref.at[m, layer + step], sems.at[layer, m])
                copy.start() if action == "start" else copy.wait()

            if step == 0:
                go()
            elif step == 1:
                pl.when(layer < layers - 1)(go)
            else:
                pl.when(layer > 0)(go)

    for layer in range(layers):
        for copy in incoming(layer):
            copy.start()

    def one(layer, carry):
        for copy in incoming(layer):
            copy.wait()
        velocity = [speed[layer, :, n * depth : (n + 1) * depth] for n in range(3)]
        density = mass[layer]
        common = common_of(velocity)
        for m in range(Q):
            value = relax(m, held[layer, m], density, velocity, common)
            value = roll(roll(value, VELOCITY_TABLE[m][1], 0), VELOCITY_TABLE[m][2], 1)
            held[layer, m] = value
        outgoing(layer, "start")
        return carry

    lax.fori_loop(0, layers, one, 0)

    def finish(layer, carry):
        outgoing(layer, "wait")
        return carry

    lax.fori_loop(0, layers, finish, 0)


def trade_kernel(x_count, y_count, *refs):
    ways = ((0, 1), (0, -1), (1, 1), (-1, -1), (1, -1), (-1, 1))
    count = len(ways)
    sources = refs[:count]
    targets, slots = refs[count + 1 : 2 * count + 1], refs[2 * count + 1 : 3 * count + 1]
    send_sem, recv_sem = refs[3 * count + 1 :]
    x = lax.axis_index("gx")
    y = lax.axis_index("gy")
    others = [(lax.rem(x + dx + x_count, x_count), lax.rem(y + dy + y_count, y_count)) for dx, dy in ways]
    barrier = pltpu.get_barrier_semaphore()
    for other in others:
        pl.semaphore_signal(barrier, inc=1, device_id=other, device_id_type=MESH)
    pl.semaphore_wait(barrier, count)
    copies = [
        pltpu.make_async_remote_copy(
            src_ref=sources[n],
            dst_ref=slots[n],
            send_sem=send_sem.at[n],
            recv_sem=recv_sem.at[n],
            device_id=others[n],
            device_id_type=MESH,
        )
        for n in range(count)
    ]
    for copy in copies:
        copy.start()
    for copy in copies:
        copy.wait()
    for n in range(count):
        targets[n][...] = slots[n][...]


def edge_kernel(whole_ref, x_low, x_high, y_low, y_high, ca, cb, cc, cd, out_ref, face, strip, face_sem, strip_sem):
    del whole_ref
    layers, rows_y = out_ref.shape[1], out_ref.shape[2]
    corners = {7: ca, 8: cb, 9: cc, 10: cd}
    copies = []
    number = 0
    for members, source, layer in ((PLUS_X, x_low, 0), (MINUS_X, x_high, layers - 1)):
        for index, m in enumerate(members):
            step_y, step_z = VELOCITY_TABLE[m][1], VELOCITY_TABLE[m][2]
            value = source[index]
            if step_y == 1:
                value = jnp.concatenate([corners[m][...], value[: rows_y - 1]], axis=0)
            elif step_y == -1:
                value = jnp.concatenate([value[1:], corners[m][...]], axis=0)
            face[number] = roll(value, step_z, 1)
            copies.append(pltpu.make_async_copy(face.at[number], out_ref.at[m, layer], face_sem.at[number]))
            number += 1
    number = 0
    for members, source, row in ((PLUS_Y, y_low, 0), (MINUS_Y, y_high, rows_y - 1)):
        for index, m in enumerate(members):
            step_x, step_z = VELOCITY_TABLE[m][0], VELOCITY_TABLE[m][2]
            strip[number] = roll(source[index], step_z, 1)
            count = layers - abs(step_x)
            source_at = 1 if step_x == -1 else 0
            target_at = 1 if step_x == 1 else 0
            copies.append(
                pltpu.make_async_copy(
                    strip.at[number, pl.ds(source_at, count)],
                    out_ref.at[m, pl.ds(target_at, count), row],
                    strip_sem.at[number],
                )
            )
            number += 1
    for copy in copies:
        copy.start()
    for copy in copies:
        copy.wait()


def shifted(value, steps_x, steps_y):
    count_x, count_y = lax.axis_size("gx"), lax.axis_size("gy")
    pairs = []
    for x in range(count_x):
        for y in range(count_y):
            target = ((x + steps_x) % count_x) * count_y + (y + steps_y) % count_y
            pairs.append((x * count_y + y, target))
    return lax.ppermute(value, ("gx", "gy"), pairs)


def local(
    populations, rotation_init, slot_cell, slot_count, marker_arm, marker_area, marker_fraction
):
    _, size_x, size_y, depth = populations.shape
    slots = marker_area.shape[2]
    planes = size_x * size_y
    shape = jax.ShapeDtypeStruct
    params = pltpu.CompilerParams(vmem_limit_bytes=VMEM_LIMIT)
    cell = slot_cell.reshape(3, slots)
    plane = (cell[0] - lax.axis_index("gx") * size_x) * size_y + cell[1] - lax.axis_index("gy") * size_y
    active = lax.broadcasted_iota(jnp.int32, (slots,), 0) < slot_count.reshape(())
    weight = jnp.where(active, marker_area.reshape(-1), 0.0)
    pack = jnp.concatenate(
        [
            plane.astype(F32)[None],
            cell[2].astype(F32)[None],
            weight[None],
            marker_fraction.reshape(1, slots),
            marker_arm.reshape(3, slots),
            jnp.zeros((1, slots), F32),
        ],
        axis=0,
    )
    held = VMEM((size_x, Q, size_y, depth), F32)
    density, velocity = pl.pallas_call(
        moments_kernel,
        in_specs=[pl.BlockSpec(memory_space=pl.ANY)],
        out_specs=[vmem(), vmem()],
        out_shape=[shape((planes, depth), F32), shape((planes, 3 * depth), F32)],
        scratch_shapes=[held, pltpu.SemaphoreType.DMA((size_x,))],
        compiler_params=params,
        name="moments",
    )(populations)
    table = VMEM((slots // 512, slots, 512), BF16)
    sums, linear = pl.pallas_call(
        gather_kernel,
        in_specs=[vmem()] * 2,
        out_specs=[vmem()] * 2,
        out_shape=[shape((8, 128), F32), shape((16, slots), F32)],
        scratch_shapes=[
            VMEM((3 * depth, planes), BF16),
            VMEM((3 * depth, planes), BF16),
            VMEM((8, slots), F32),
            VMEM((8, slots), F32),
            VMEM((slots, 128), F32),
            VMEM((slots, 128), F32),
            table,
            table,
            table,
            VMEM((48, slots), BF16),
        ],
        compiler_params=params,
        name="gather",
    )(velocity, pack)
    count_x, count_y = lax.axis_size("gx"), lax.axis_size("gy")
    dma = pltpu.SemaphoreType.DMA
    sums = pl.pallas_call(
        functools.partial(total_kernel, count_x, count_y),
        in_specs=[vmem()],
        out_specs=vmem(),
        out_shape=shape((8, 128), F32),
        scratch_shapes=[
            VMEM((count_y - 1, 8, 128), F32),
            VMEM((8, 128), F32),
            VMEM((count_x - 1, 8, 128), F32),
            dma((count_y - 1,)),
            dma((count_y - 1,)),
            dma((count_x - 1,)),
            dma((count_x - 1,)),
        ],
        compiler_params=pltpu.CompilerParams(collective_id=0, has_side_effects=True),
        name="total",
    )(sums)
    x_face = shape((len(PLUS_X), size_y, depth), F32)
    y_face = shape((len(PLUS_Y), size_x, depth), F32)
    corner = shape((1, depth), F32)
    moved, spins, x_up, x_down, y_up, y_down, c7, c8, c9, c10 = pl.pallas_call(
        functools.partial(spread_kernel, size_y),
        in_specs=[vmem()] * 6 + [pl.BlockSpec(memory_space=pl.ANY)],
        out_specs=[vmem()] * 10,
        out_shape=[
            shape((planes, 3 * depth), F32),
            shape((ITERS, 3), F32),
            x_face,
            x_face,
            y_face,
            y_face,
            corner,
            corner,
            corner,
            corner,
        ],
        scratch_shapes=[
            VMEM((planes, slots), BF16),
            VMEM((3 * depth, slots), BF16),
            VMEM((3 * depth, slots), BF16),
            VMEM((2 * len(PLUS_X), size_y, depth), F32),
            VMEM((2 * len(PLUS_Y), size_x, depth), F32),
            VMEM((128, 128), F32),
            dma((2 * len(PLUS_X),)),
            dma((2 * len(PLUS_Y),)),
        ],
        compiler_params=params,
        name="spread",
    )(rotation_init.reshape(1, 3), sums, linear, pack, velocity, density, populations)
    x_low = shifted(x_up, 1, 0)
    x_high = shifted(x_down, -1, 0)
    whole = pl.pallas_call(
        functools.partial(collide_kernel, size_x),
        in_specs=[pl.BlockSpec(memory_space=pl.ANY)] * 3,
        out_specs=pl.BlockSpec(memory_space=pl.ANY),
        out_shape=shape(populations.shape, F32),
        scratch_shapes=[
            held,
            VMEM((size_x, size_y, 3 * depth), F32),
            VMEM((size_x, size_y, depth), F32),
            dma((3, size_x)),
            dma((size_x, Q)),
        ],
        compiler_params=params,
        cost_estimate=pl.CostEstimate(flops=100_000_000, bytes_accessed=20_000_000, transcendentals=0),
        name="collide",
    )(populations, moved, density)
    small = [y_face, y_face, corner, corner, corner, corner]
    y_low, y_high, c7, c8, c9, c10 = pl.pallas_call(
        functools.partial(trade_kernel, count_x, count_y),
        in_specs=[vmem()] * 6 + [pl.BlockSpec(memory_space=pl.ANY)],
        out_specs=[vmem()] * 6,
        out_shape=small,
        scratch_shapes=[VMEM(one.shape, F32) for one in small] + [dma((6,)), dma((6,))],
        compiler_params=pltpu.CompilerParams(collective_id=1, has_side_effects=True),
        cost_estimate=pl.CostEstimate(flops=20_000_000, bytes_accessed=1_000_000, transcendentals=0),
        name="trade",
    )(y_up, y_down, c7, c8, c9, c10, whole)
    whole = pl.pallas_call(
        edge_kernel,
        in_specs=[pl.BlockSpec(memory_space=pl.ANY)] + [vmem()] * 8,
        out_specs=pl.BlockSpec(memory_space=pl.ANY),
        out_shape=shape(populations.shape, F32),
        scratch_shapes=[
            VMEM((2 * len(PLUS_X), size_y, depth), F32),
            VMEM((2 * len(PLUS_Y), size_x, depth), F32),
            dma((2 * len(PLUS_X),)),
            dma((2 * len(PLUS_Y),)),
        ],
        input_output_aliases={0: 0},
        name="edges",
    )(whole, x_low, x_high, y_low, y_high, c7, c8, c9, c10)
    return whole, spins


def solution(mesh):
    return jax.shard_map(
        local,
        mesh=mesh,
        in_specs=(
            P(None, "gx", "gy", None),
            P(),
            P(None, "gx", "gy", None),
            P("gx", "gy"),
            P(None, "gx", "gy", None),
            P("gx", "gy", None),
            P("gx", "gy", None),
        ),
        out_specs=(P(None, "gx", "gy", None), P()),
        check_vma=False,
    )
```
